128 devices in a mesh: cp: 32 (over y, z, core), ep: 4 (over x).
Axes of the slice: x: 4, y: 4, z: 4, core: 2. Of those that a mesh axis runs over, the one named last changes fastest.
Arguments:
- residual: bfloat16 [4096, 6144], P('cp'), may hold values from -90 to 90
- queries: bfloat16 [4096, 3072], P('cp', 'ep'), may hold values from -256 to 256
- key_proj: bfloat16 [4096, 512], P('cp', 'ep'), may hold values from -8 to 8
- value_proj: bfloat16 [4096, 512], P('cp', 'ep'), may hold values from -12 to 12
- out_weight: bfloat16 [3072, 6144], P('ep'), may hold values from -0.109375 to 0.109375
- norm_gain: float32 [6144], replicated, may hold values from 0.1 to 1.9
- doc_ids: int32 [4096], replicated, may hold values from 0 to 11, never falling along the last dimension, each value on 1 to 1024 neighbouring positions
- block_order: int32 [32], replicated, may hold values from 0 to 31, each once
- expert_ids: int32 [4096, 2], P('cp'), may hold values from 0 to 7, as said below
- route_logits: float32 [4096, 2], P('cp'), may hold values from -12 to 12
- gate_weight: bfloat16 [4, 6144, 8192], P('ep', None, 'cp'), may hold values from -0.078125 to 0.078125
- up_weight: bfloat16 [4, 6144, 8192], P('ep', None, 'cp'), may hold values from -0.078125 to 0.078125
- down_weight: bfloat16 [4, 8192, 6144], P('ep', 'cp'), may hold values from -0.0625 to 0.0625
Outputs:
- hidden_state: bfloat16 [4096, 6144], P('cp', 'ep')
- expert_mix: bfloat16 [4096, 6144], P('cp', 'ep')
The draws below stay inside these ranges and needn't reach their ends.
Inputs may be any that keep to these rules, and one draw needn't show every extreme that they name: `expert_ids`: each row names two different experts; within the 128 rows of one cp index no expert is named by more than 40 rows. `doc_ids`: document numbers never fall along the sequence. `block_order`: each block number appears once.
All inputs are finite; a program needn't handle non-finite values.
Results may differ from the reference program's by a relative error of at most 0.02.
Values may be sent and summed in bfloat16 or wider, within the bound.
No kernel may reach another device: no remote copies, remote signals or barrier semaphores. Data moves between devices by JAX's collectives and lax.ppermute only.
A program may use at most 128 MiB of HBM per device.

```python
import math
import jax
import jax.numpy as jnp
import numpy as np
from jax import lax

D = 6144
HD = 128
EXPERTS = 8
QH = 24
KVH = 4
FFW = 8192
DOCS = 12
TOK_DEV = 128
SEQ = 4096
CAP = 40
EXP_WIN = 4
N_CP = 32


def key_base(key):
    return jax.random.truncated_normal(jax.random.fold_in(key, 31), -6.0, 6.0, (SEQ, KVH, HD), jnp.float32)


def draw_key_proj(key, part):
    base = key_base(key)
    return base.reshape(SEQ, KVH * HD).astype(jnp.bfloat16)


def draw_queries(key, part):
    base = jax.random.truncated_normal(jax.random.fold_in(key, 41), -6.0, 6.0, (SEQ, QH, HD), jnp.float32)
    return base.reshape(SEQ, QH * HD).astype(jnp.bfloat16)


def draw_residual(key, part):
    base = jax.random.truncated_normal(jax.random.fold_in(key, 21), -6.0, 6.0, (SEQ, D), jnp.float32)
    return base.astype(jnp.bfloat16)


def draw_expert_ids(key, part):
    blocks = SEQ // TOK_DEV
    filled = jax.random.randint(jax.random.fold_in(key, 3), (), 0, EXP_WIN, dtype=jnp.int32)
    others = EXPERTS - 2
    remaining = 2 * TOK_DEV - 2 * CAP
    expert_range = jnp.arange(EXPERTS, dtype=jnp.int32)
    entry_range = jnp.arange(2 * TOK_DEV, dtype=jnp.int32)

    def one_block(block_key):
        first_key, second_key, third_key, fourth_key = jax.random.split(block_key, 4)
        second = (filled + 1 + jax.random.randint(first_key, (), 0, EXPERTS - 1, dtype=jnp.int32)) % EXPERTS
        is_top = (expert_range == filled) | (expert_range == second)
        other_rank = jnp.clip(jnp.cumsum(1 - is_top.astype(jnp.int32)) - 1, 0, others - 1)
        ordering = jax.random.permutation(second_key, others)
        extra = (ordering[other_rank] < remaining % others).astype(jnp.int32)
        counts = jnp.where(is_top, CAP, remaining // others + extra).astype(jnp.int32)
        bounds = jnp.cumsum(counts)
        entries = jnp.sum((entry_range[:, None] >= bounds[None, :]).astype(jnp.int32), axis=1)
        paired = jnp.stack([entries[:TOK_DEV], entries[TOK_DEV:]], axis=1)
        paired = paired[jax.random.permutation(third_key, TOK_DEV)]
        flipped = jax.random.randint(fourth_key, (TOK_DEV, 1), 0, 2, dtype=jnp.int32)
        return jnp.where(flipped == 1, paired[:, ::-1], paired)
    block_keys = jax.random.split(jax.random.fold_in(key, 5), blocks)
    return jax.vmap(one_block)(block_keys).reshape(SEQ, 2).astype(jnp.int32)


def shard_levels(rng, dims, pieces, low, top_value):
    level, own = 1.0, jax.random.fold_in(rng, 6)
    for axis_at, shards_of in pieces:
        heights = jnp.exp(jax.random.uniform(jax.random.fold_in(own, axis_at), (shards_of,), jnp.float32, low / len(pieces), top_value / len(pieces)))
        level = level * jnp.repeat(heights, dims[axis_at] // shards_of).reshape([-1 if axis == axis_at else 1 for axis in range(len(dims))])
    return level


def length_profile(number_of, total, most, slope):
    weights = [(1 << 20) // math.isqrt(grade ** slope) + 1 for grade in range(2, number_of + 1)]
    surplus, given = total - most - (number_of - 1), [1] * (number_of - 1)
    while surplus > 0:
        movable = [i for i in range(number_of - 1) if given[i] < most]
        mass, budget = sum([weights[i] for i in movable]), surplus
        for i in movable:
            more = min(most - given[i], max(1, budget * weights[i] // mass), surplus)
            given[i] = given[i] + more
            surplus = surplus - more
    return np.array([most] + given)


def ragged(own_key, amount, total, bound, skew):
    if amount == 2:
        one = jax.random.randint(own_key, (), max(1, total - bound), min(bound, total - 1) + 1)
        return jnp.stack([one, total - one])
    tallies = jnp.asarray(length_profile(amount, total, bound, skew), jnp.int32)
    pairs = (amount - 1) // 2
    donor, sink = tallies[1:1 + 2 * pairs:2], tallies[2:2 + 2 * pairs:2]
    room = jnp.minimum(donor - 1, bound - sink)
    passed = jax.random.randint(jax.random.fold_in(own_key, 1), (pairs,), 0, 1 << 20) % (room + 1)
    tallies = tallies.at[1:1 + 2 * pairs:2].set(donor - passed).at[2:2 + 2 * pairs:2].set(sink + passed)
    return tallies[jax.random.permutation(jax.random.fold_in(own_key, 2), amount)]


def centred(key, shape, width, limit, cuts=(), kind=jnp.bfloat16):
    loudness = shard_levels(key, shape, cuts, -0.22, 0.18) if cuts else 1.0
    values = jax.random.normal(key, shape, jnp.float32) * width * loudness
    return jnp.minimum(jnp.maximum(values, -limit), limit).astype(kind)


def setup_inputs(seed: int = 0) -> dict:
    key_list = jax.random.split(jax.random.key(seed), 14)
    residual = draw_residual(jax.random.fold_in(key_list[13], 71), 0)
    queries = draw_queries(jax.random.fold_in(key_list[13], 71), 0)
    key_proj = draw_key_proj(jax.random.fold_in(key_list[13], 71), 0)
    value_proj = centred(key_list[3], (SEQ, KVH * HD), 2.0, 12.0, ((0, 32), (1, 4)))
    out_weight = centred(key_list[4], (QH * HD, D), (QH * HD) ** -0.5, 0.109375, ((0, 4),))
    norm_gain = jnp.clip(1.0 + 0.18 * jax.random.normal(key_list[5], (D,), jnp.float32), 0.1, 1.9)
    doc_ids = jnp.searchsorted(jnp.cumsum(ragged(key_list[6], DOCS, SEQ, SEQ // 4, 2)), jnp.arange(SEQ), side="right").astype(jnp.int32)
    block_order = jax.random.permutation(key_list[7], N_CP).astype(jnp.int32)
    expert_ids = draw_expert_ids(jax.random.fold_in(key_list[13], 71), 0)
    route_logits = centred(key_list[9], (SEQ, 2), 2.0, 12.0, ((0, 32),), jnp.float32)
    gate_weight = centred(key_list[10], (EXP_WIN, D, FFW), D ** -0.5, 0.078125, ((0, 4), (2, 32)))
    up_weight = centred(key_list[11], (EXP_WIN, D, FFW), D ** -0.5, 0.078125, ((0, 4), (2, 32)))
    down_weight = centred(key_list[12], (EXP_WIN, FFW, D), FFW ** -0.5, 0.0625, ((0, 4), (1, 32)))
    return {"residual": residual, "queries": queries, "key_proj": key_proj, "value_proj": value_proj, "out_weight": out_weight, "norm_gain": norm_gain, "doc_ids": doc_ids, "block_order": block_order, "expert_ids": expert_ids, "route_logits": route_logits, "gate_weight": gate_weight, "up_weight": up_weight, "down_weight": down_weight}


EPS = 1e-05
NEG = -1e+30

def reference(residual, queries, key_proj, value_proj, out_weight, norm_gain, doc_ids, block_order, expert_ids, route_logits, gate_weight, up_weight, down_weight):
    positions = (block_order[:, None] * TOK_DEV + jnp.arange(TOK_DEV, dtype=jnp.int32)[None, :]).reshape(SEQ).astype(jnp.int32)
    row_docs = jnp.take(doc_ids, positions)
    allowed = (row_docs[:, None] == row_docs[None, :]) & (positions[None, :] <= positions[:, None])
    group_size = QH // KVH
    score_scale = 1.0 / math.sqrt(HD)
    query_heads = queries.reshape(SEQ, QH, HD)
    key_heads = key_proj.reshape(SEQ, KVH, HD)
    value_heads = value_proj.reshape(SEQ, KVH, HD)

    def one_head(head_index):
        query_rows = lax.dynamic_index_in_dim(query_heads, head_index, 1, keepdims=False)
        key_rows = lax.dynamic_index_in_dim(key_heads, head_index // group_size, 1, keepdims=False)
        value_rows = lax.dynamic_index_in_dim(value_heads, head_index // group_size, 1, keepdims=False)
        scores = lax.dot_general(query_rows, key_rows, (((1,), (1,)), ((), ())), preferred_element_type=jnp.float32) * score_scale
        scores = jnp.where(allowed, scores, NEG)
        row_max = lax.optimization_barrier(jnp.max(scores, axis=1, keepdims=True))
        weights = jnp.where(allowed, jnp.exp(scores - row_max), 0.0)
        row_total = lax.optimization_barrier(jnp.sum(weights, axis=1, keepdims=True))
        value_mix = jnp.dot(weights.astype(jnp.bfloat16), value_rows, preferred_element_type=jnp.float32)
        return value_mix / row_total
    attended = lax.map(one_head, jnp.arange(QH, dtype=jnp.int32))
    attended = attended.transpose(1, 0, 2).reshape(SEQ, QH * HD).astype(jnp.bfloat16)
    projected = jnp.dot(attended, out_weight, preferred_element_type=jnp.float32)
    hidden_state = (residual.astype(jnp.float32) + projected).astype(jnp.bfloat16)
    values_wide = hidden_state.astype(jnp.float32)
    mean_square = lax.optimization_barrier(jnp.mean(values_wide * values_wide, axis=1, keepdims=True))
    normed = (values_wide * lax.rsqrt(mean_square + EPS) * norm_gain).astype(jnp.bfloat16)
    logit_gap = route_logits[:, 1] - route_logits[:, 0]
    first_share = 1.0 / (1.0 + jnp.exp(logit_gap))
    second_share = 1.0 / (1.0 + jnp.exp(-logit_gap))
    slice_width = FFW // N_CP
    block_normed = normed.reshape(N_CP, TOK_DEV, D).astype(jnp.float32)
    slot_ids = jnp.arange(CAP, dtype=jnp.int32)
    block_base = jnp.arange(SEQ, dtype=jnp.int32) // TOK_DEV * CAP
    mixture = jnp.zeros((SEQ, D), jnp.float32)
    for expert in range(EXP_WIN):
        is_member = ((expert_ids[:, 0] == expert) | (expert_ids[:, 1] == expert)).astype(jnp.int32)
        member_blocks = is_member.reshape(N_CP, TOK_DEV)
        slot_index = jnp.cumsum(member_blocks, axis=1) - member_blocks
        selector = ((slot_index[:, None, :] == slot_ids[None, :, None]) & (member_blocks[:, None, :] == 1)).astype(jnp.float32)
        packed = jnp.einsum('bct,btd->bcd', selector, block_normed).astype(jnp.bfloat16).reshape(N_CP * CAP, D)
        gated = jnp.dot(packed, gate_weight[expert], preferred_element_type=jnp.float32)
        lifted = jnp.dot(packed, up_weight[expert], preferred_element_type=jnp.float32)
        hidden = (jax.nn.silu(gated) * lifted).astype(jnp.bfloat16)
        hidden_slices = hidden.reshape(N_CP * CAP, N_CP, slice_width).transpose(1, 0, 2)
        down_slices = down_weight[expert].reshape(N_CP, slice_width, D)

        def add_slice(running, pair):
            term = jnp.dot(pair[0], pair[1], preferred_element_type=jnp.float32).astype(jnp.bfloat16)
            term = lax.optimization_barrier(term)
            return (running + term.astype(jnp.float32), None)
        expert_sum, unused = lax.scan(add_slice, jnp.zeros((N_CP * CAP, D), jnp.float32), (hidden_slices, down_slices))
        route_share = jnp.where(expert_ids[:, 0] == expert, first_share, 0.0) + jnp.where(expert_ids[:, 1] == expert, second_share, 0.0)
        row_index = (block_base + jnp.minimum(slot_index.reshape(SEQ), CAP - 1)).astype(jnp.int32)
        mixture = mixture + jnp.take(expert_sum, row_index, axis=0) * route_share[:, None]
    return (hidden_state, mixture.astype(jnp.bfloat16))
```

```python
import math

import jax
import jax.numpy as jnp
from jax import lax
from jax.experimental import pallas as pl
from jax.experimental.pallas import tpu as pltpu
from jax.sharding import PartitionSpec as P

HD = 128
CAP = 40
EPS = 1e-05
NEG = -1e30
SIDE = 4
WINDOW = 9


def device_at(y, z, core):
    return ((y % SIDE) * SIDE + z % SIDE) * 2 + core % 2


def shifted(array, dy, dz, dcore=0):
    pairs = [
        (device_at(y, z, c), device_at(y + dy, z + dz, c + dcore))
        for y in range(SIDE)
        for z in range(SIDE)
        for c in range(2)
    ]
    return lax.ppermute(array, "cp", pairs)


def along(array, dim, step):
    return shifted(array, step, 0) if dim == "y" else shifted(array, 0, step)


def gather_line(array, dim):
    return [array] + [along(array, dim, step) for step in (1, 2, 3)]


def attention_kernel(slots_ref, q_ref, own_ref, other_ref, row_doc_ref, key_doc_ref, out_ref, kv_ref):
    tokens = q_ref.shape[0]
    heads = q_ref.shape[1] // HD
    half = own_ref.shape[0] // tokens
    for w in range(WINDOW):
        slot = slots_ref[w]

        @pl.when(slot < half)
        def _():
            kv_ref[w * tokens : (w + 1) * tokens, :] = own_ref[pl.ds(slot * tokens, tokens), :]

        @pl.when(slot >= half)
        def _():
            kv_ref[w * tokens : (w + 1) * tokens, :] = other_ref[
                pl.ds((slot - half) * tokens, tokens), :
            ]

    width = WINDOW * tokens
    key_at = lax.broadcasted_iota(jnp.int32, (tokens, width), 1) - (WINDOW - 1) * tokens
    row_at = lax.broadcasted_iota(jnp.int32, (tokens, width), 0)
    allowed = (key_doc_ref[...] == row_doc_ref[...]) & (key_at <= row_at)
    keys = kv_ref[:, :HD]
    values = kv_ref[:, HD:]
    for h in range(heads):
        scores = lax.dot_general(
            q_ref[:, h * HD : (h + 1) * HD],
            keys,
            (((1,), (1,)), ((), ())),
            preferred_element_type=jnp.float32,
        ) * (1.0 / math.sqrt(HD))
        scores = jnp.where(allowed, scores, NEG)
        top = jnp.max(scores, axis=1, keepdims=True)
        weights = jnp.where(allowed, jnp.exp(scores - top), 0.0)
        total = jnp.sum(weights, axis=1, keepdims=True)
        mix = jnp.dot(weights.astype(jnp.bfloat16), values, preferred_element_type=jnp.float32)
        out_ref[:, h * HD : (h + 1) * HD] = (mix / total).astype(jnp.bfloat16)


def attend(slots, queries, own, other, row_docs, key_docs):
    vmem = pl.BlockSpec(memory_space=pltpu.VMEM)
    return pl.pallas_call(
        attention_kernel,
        out_shape=jax.ShapeDtypeStruct(queries.shape, jnp.bfloat16),
        in_specs=[pl.BlockSpec(memory_space=pltpu.SMEM)] + [vmem] * 5,
        out_specs=vmem,
        scratch_shapes=[pltpu.VMEM((WINDOW * queries.shape[0], 2 * HD), jnp.bfloat16)],
        name="attention",
    )(slots, queries, own, other, row_docs, key_docs)


def local(
    residual,
    queries,
    key_proj,
    value_proj,
    out_weight,
    norm_gain,
    doc_ids,
    block_order,
    expert_ids,
    route_logits,
    gate_weight,
    up_weight,
    down_weight,
):
    tokens, width = residual.shape
    quarter = width // SIDE
    half = width // 2
    cp_rank = lax.axis_index("cp")
    ep_rank = lax.axis_index("ep")
    core = cp_rank % 2
    z = (cp_rank // 2) % SIDE
    y = cp_rank // (2 * SIDE)

    gate_other = shifted(gate_weight[0], 0, 0, 1)
    up_other = shifted(up_weight[0], 0, 0, 1)
    down_other = shifted(down_weight[0], 0, 0, 1)

    kv = jnp.concatenate([key_proj, value_proj], axis=1)
    kv_line = jnp.concatenate(gather_line(kv, "y"), axis=0)
    kv_own = jnp.concatenate(gather_line(kv_line, "z"), axis=0)
    kv_other = shifted(kv_own, 0, 0, 1)

    slot = jnp.arange(2 * SIDE * SIDE, dtype=jnp.int32)
    slot_core = jnp.where(slot < SIDE * SIDE, core, 1 - core)
    slot_y = (y - slot % SIDE) % SIDE
    slot_z = (z - (slot // SIDE) % SIDE) % SIDE
    source = (slot_y * SIDE + slot_z) * 2 + slot_core
    slot_block = jnp.sum(
        jnp.where(source[:, None] == slot[None, :], block_order[None, :], 0), axis=1
    )
    placed = jnp.sum(jnp.where(slot == cp_rank, block_order, 0))
    wanted = placed - (WINDOW - 1) + jnp.arange(WINDOW, dtype=jnp.int32)
    slots = jnp.sum(jnp.where(wanted[:, None] == slot_block[None, :], slot[None, :], 0), axis=1)
    before = jnp.full(((WINDOW - 1) * tokens,), -1, jnp.int32)
    key_docs = lax.dynamic_slice_in_dim(
        jnp.concatenate([before, doc_ids]), placed * tokens, WINDOW * tokens
    )
    row_docs = key_docs[(WINDOW - 1) * tokens :]
    attended = attend(slots, queries, kv_own, kv_other, row_docs[:, None], key_docs[None, :])

    projected = jnp.dot(attended, out_weight, preferred_element_type=jnp.float32)
    projected = projected.astype(jnp.bfloat16).reshape(tokens, SIDE, quarter).transpose(1, 0, 2)
    arrived = lax.all_to_all(projected, "ep", split_axis=0, concat_axis=0, tiled=True)
    own_residual = lax.dynamic_slice_in_dim(residual, ep_rank * quarter, quarter, 1)
    hidden_state = (
        own_residual.astype(jnp.float32) + arrived.astype(jnp.float32).sum(axis=0)
    ).astype(jnp.bfloat16)

    experts = jnp.arange(SIDE, dtype=jnp.int32)
    logit_gap = route_logits[:, 1] - route_logits[:, 0]
    first_share = 1.0 / (1.0 + jnp.exp(logit_gap))
    second_share = 1.0 / (1.0 + jnp.exp(-logit_gap))
    names_first = expert_ids[:, 0][:, None] == experts[None, :]
    names_second = expert_ids[:, 1][:, None] == experts[None, :]
    member = (names_first | names_second).astype(jnp.int32)
    slot_index = jnp.cumsum(member, axis=0) - member
    share = jnp.where(names_first, first_share[:, None], 0.0) + jnp.where(
        names_second, second_share[:, None], 0.0
    )
    slot_ids = jnp.arange(CAP, dtype=jnp.int32)
    placed_at = (slot_index[:, :, None] == slot_ids[None, None, :]) & (member[:, :, None] == 1)
    selector = placed_at.astype(jnp.bfloat16).reshape(tokens, SIDE * CAP)
    mix_weight = jnp.where(placed_at, share[:, :, None], 0.0).reshape(tokens, SIDE * CAP)

    rows = lax.dot_general(
        selector, hidden_state, (((0,), (0,)), ((), ())), preferred_element_type=jnp.float32
    ).astype(jnp.bfloat16)
    rows = lax.all_to_all(
        rows.reshape(SIDE, CAP, quarter), "ep", split_axis=0, concat_axis=0, tiled=True
    )
    wide = rows.astype(jnp.float32)
    mean_square = jnp.sum(wide * wide, axis=(0, 2), keepdims=True) / width
    gain = norm_gain.reshape(SIDE, 1, quarter)
    packed = (wide * lax.rsqrt(mean_square + EPS) * gain).astype(jnp.bfloat16)
    first = jnp.concatenate([packed[0], packed[1]], axis=1)
    second = jnp.concatenate([packed[2], packed[3]], axis=1)

    first_line = jnp.concatenate(gather_line(first, "y"), axis=0)
    second_line = jnp.concatenate(gather_line(second, "z"), axis=0)
    first_all = jnp.concatenate(gather_line(first_line, "z"), axis=0)
    second_all = jnp.concatenate(gather_line(second_line, "y"), axis=0)

    gate_up = jnp.concatenate([gate_weight[0], gate_other, up_weight[0], up_other], axis=1)
    down = jnp.concatenate([down_weight[0], down_other], axis=0)
    units = down.shape[0]
    from_first = jnp.dot(first_all, gate_up[:half], preferred_element_type=jnp.float32)
    from_second = jnp.dot(second_all, gate_up[half:], preferred_element_type=jnp.float32)

    def swapped(array):
        shape = (SIDE, SIDE, CAP, array.shape[1])
        return array.reshape(shape).transpose(1, 0, 2, 3).reshape(array.shape)

    lifted = from_first + swapped(from_second)
    hidden = (jax.nn.silu(lifted[:, :units]) * lifted[:, units:]).astype(jnp.bfloat16)
    partial_first = jnp.dot(hidden, down[:, :half], preferred_element_type=jnp.float32).astype(
        jnp.bfloat16
    )
    partial_second = jnp.dot(
        swapped(hidden), down[:, half:], preferred_element_type=jnp.float32
    ).astype(jnp.bfloat16)

    def scatter_line(array, dim):
        pieces = array.reshape(SIDE, -1, array.shape[1])
        total = pieces[0].astype(jnp.float32)
        for step in (1, 2, 3):
            total = total + along(pieces[step], dim, -step).astype(jnp.float32)
        return total.astype(jnp.bfloat16)

    sum_first = scatter_line(scatter_line(partial_first, "z"), "y")
    sum_second = scatter_line(scatter_line(partial_second, "y"), "z")
    back = jnp.stack(
        [sum_first[:, :quarter], sum_first[:, quarter:], sum_second[:, :quarter], sum_second[:, quarter:]]
    )
    back = lax.all_to_all(back, "ep", split_axis=0, concat_axis=0, tiled=True)
    back = back.reshape(SIDE * CAP, quarter)
    high = mix_weight.astype(jnp.bfloat16)
    low = (mix_weight - high.astype(jnp.float32)).astype(jnp.bfloat16)
    mixed = jnp.dot(high, back, preferred_element_type=jnp.float32) + jnp.dot(
        low, back, preferred_element_type=jnp.float32
    )
    return (hidden_state, mixed.astype(jnp.bfloat16))


def solution(mesh):
    return jax.shard_map(
        local,
        mesh=mesh,
        in_specs=(
            P("cp", None),
            P("cp", "ep"),
            P("cp", "ep"),
            P("cp", "ep"),
            P("ep", None),
            P(),
            P(),
            P(),
            P("cp", None),
            P("cp", None),
            P("ep", None, "cp"),
            P("ep", None, "cp"),
            P("ep", "cp", None),
        ),
        out_specs=(P("cp", "ep"), P("cp", "ep")),
        check_vma=False,
    )
```

```python
import math

import jax
import jax.numpy as jnp
from jax import lax
from jax.experimental import pallas as pl
from jax.experimental.pallas import tpu as pltpu
from jax.sharding import PartitionSpec as P

HD = 128
CAP = 40
EPS = 1e-05
NEG = -1e30
SIDE = 4
WINDOW = 9


def device_at(y, z, core):
    return ((y % SIDE) * SIDE + z % SIDE) * 2 + core % 2


def shifted(array, dy, dz, dcore=0):
    pairs = [
        (device_at(y, z, c), device_at(y + dy, z + dz, c + dcore))
        for y in range(SIDE)
        for z in range(SIDE)
        for c in range(2)
    ]
    return lax.ppermute(array, "cp", pairs)


def along(array, dim, step):
    return shifted(array, step, 0) if dim == "y" else shifted(array, 0, step)


def gather_line(array, dim):
    return [array] + [along(array, dim, step) for step in (1, 2, 3)]


def attention_kernel(
    rank_ref, order_ref, q_ref, own_ref, other_ref, docs_ref, weight_hbm, out_ref,
    kv_ref, bias_ref, attended_ref, weight_ref, sems,
):
    tokens = q_ref.shape[0]
    heads = q_ref.shape[1] // HD
    quarters, _, quarter = out_ref.shape

    def fetch(j):
        return pltpu.make_async_copy(
            weight_hbm.at[:, pl.ds(j * quarter, quarter)], weight_ref.at[j], sems.at[j]
        )

    for j in range(quarters):
        fetch(j).start()

    rank = rank_ref[0]
    core = rank % 2
    z = (rank // 2) % SIDE
    y = rank // (2 * SIDE)
    placed = order_ref[rank]
    first_block = placed - (WINDOW - 1)
    for slot in range(2 * SIDE * SIDE):
        in_half = slot % (SIDE * SIDE)
        slot_core = core if slot < SIDE * SIDE else 1 - core
        slot_y = (y + SIDE - in_half % SIDE) % SIDE
        slot_z = (z + SIDE - in_half // SIDE) % SIDE
        at = order_ref[(slot_y * SIDE + slot_z) * 2 + slot_core] - first_block
        source = own_ref if slot < SIDE * SIDE else other_ref

        @pl.when((at >= 0) & (at < WINDOW))
        def _():
            kv_ref[pl.ds(pl.multiple_of(at * tokens, tokens), tokens), :] = source[
                in_half * tokens : (in_half + 1) * tokens, :
            ]

    row_at = lax.broadcasted_iota(jnp.int32, (tokens, tokens), 0)
    key_at = lax.broadcasted_iota(jnp.int32, (tokens, tokens), 1)
    own_docs = docs_ref[pl.ds(placed, 1), :]
    row_docs = jnp.sum(jnp.where(row_at == key_at, own_docs, 0), axis=1, keepdims=True)
    for w in range(WINDOW):
        block = first_block + w

        @pl.when(block < 0)
        def _():
            kv_ref[w * tokens : (w + 1) * tokens, :] = jnp.zeros((tokens, 2 * HD), jnp.bfloat16)

        allowed = docs_ref[pl.ds(jnp.maximum(block, 0), 1), :] == row_docs
        allowed = allowed & (key_at + (w - (WINDOW - 1)) * tokens <= row_at)
        allowed = allowed & (jnp.full((tokens, tokens), block, jnp.int32) >= 0)
        bias_ref[:, w * tokens : (w + 1) * tokens] = jnp.where(allowed, 0.0, NEG)

    keys = kv_ref[:, :HD]
    values = kv_ref[:, HD:]
    for h in range(heads):
        scores = lax.dot_general(
            q_ref[:, h * HD : (h + 1) * HD],
            keys,
            (((1,), (1,)), ((), ())),
            preferred_element_type=jnp.float32,
        )
        scores = scores * (1.0 / math.sqrt(HD)) + bias_ref[...]
        weights = jnp.exp(scores - jnp.max(scores, axis=1, keepdims=True))
        total = jnp.sum(weights, axis=1, keepdims=True)
        mix = jnp.dot(weights.astype(jnp.bfloat16), values, preferred_element_type=jnp.float32)
        attended_ref[:, h * HD : (h + 1) * HD] = (mix / total).astype(jnp.bfloat16)
    for j in range(quarters):
        fetch(j).wait()
        out_ref[j] = jnp.dot(
            attended_ref[...], weight_ref[j], preferred_element_type=jnp.float32
        ).astype(jnp.bfloat16)


def attend_and_project(rank, order, queries, own, other, docs, out_weight):
    tokens, inner = queries.shape
    quarter = out_weight.shape[1] // SIDE
    smem = pl.BlockSpec(memory_space=pltpu.SMEM)
    vmem = pl.BlockSpec(memory_space=pltpu.VMEM)
    return pl.pallas_call(
        attention_kernel,
        out_shape=jax.ShapeDtypeStruct((SIDE, tokens, quarter), jnp.bfloat16),
        in_specs=[smem, smem, vmem, vmem, vmem, vmem, pl.BlockSpec(memory_space=pl.ANY)],
        out_specs=vmem,
        scratch_shapes=[
            pltpu.VMEM((WINDOW * tokens, 2 * HD), jnp.bfloat16),
            pltpu.VMEM((tokens, WINDOW * tokens), jnp.float32),
            pltpu.VMEM((tokens, inner), jnp.bfloat16),
            pltpu.VMEM((SIDE, inner, quarter), jnp.bfloat16),
            pltpu.SemaphoreType.DMA((SIDE,)),
        ],
        compiler_params=pltpu.CompilerParams(vmem_limit_bytes=40 * 1024 * 1024),
        name="attention",
    )(rank, order, queries, own, other, docs, out_weight)


def gather_ring(near, far, dim):
    up_near = along(near, dim, 1)
    down_far = along(far, dim, -1)
    up_far = along(far, dim, 1)
    down_near = along(near, dim, -1)
    two_near = along(up_near, dim, 1)
    two_far = along(down_far, dim, -1)
    return [(near, far), (up_near, up_far), (two_near, two_far), (down_near, down_far)]


def plus(*arrays):
    total = arrays[0].astype(jnp.float32)
    for a in arrays[1:]:
        total = total + a.astype(jnp.float32)
    return total.astype(jnp.bfloat16)


def scatter_ring(pieces, dim):
    near2 = along(pieces[2][0], dim, -1)
    far2 = along(pieces[2][1], dim, 1)
    far1 = along(pieces[1][1], dim, -1)
    near3 = along(pieces[3][0], dim, 1)
    near1 = along(plus(pieces[1][0], near2), dim, -1)
    far3 = along(plus(pieces[3][1], far2), dim, 1)
    return plus(pieces[0][0], near3, near1), plus(pieces[0][1], far1, far3)


def scatter_line(near, far, dim):
    rows = near.shape[0] // 2
    pieces = [near[:rows], near[rows:], far[:rows], far[rows:]]
    return plus(pieces[0], *[along(pieces[step], dim, -step) for step in (1, 2, 3)])


def local(
    residual,
    queries,
    key_proj,
    value_proj,
    out_weight,
    norm_gain,
    doc_ids,
    block_order,
    expert_ids,
    route_logits,
    gate_weight,
    up_weight,
    down_weight,
):
    tokens, width = residual.shape
    quarter = width // SIDE
    half = width // 2
    cp_rank = lax.axis_index("cp")
    ep_rank = lax.axis_index("ep")

    gate_other = shifted(gate_weight[0], 0, 0, 1)
    up_other = shifted(up_weight[0], 0, 0, 1)
    down_other = shifted(down_weight[0], 0, 0, 1)

    kv = jnp.concatenate([key_proj, value_proj], axis=1)
    kv_line = jnp.concatenate(gather_line(kv, "y"), axis=0)
    kv_own = jnp.concatenate(gather_line(kv_line, "z"), axis=0)
    kv_other = shifted(kv_own, 0, 0, 1)

    projected = attend_and_project(
        cp_rank.reshape(1).astype(jnp.int32),
        block_order,
        queries,
        kv_own,
        kv_other,
        doc_ids.reshape(-1, tokens),
        out_weight,
    )
    gate_up = jnp.concatenate([gate_weight[0], gate_other, up_weight[0], up_other], axis=1)
    down = jnp.concatenate([down_weight[0], down_other], axis=0)
    arrived = lax.all_to_all(projected, "ep", split_axis=0, concat_axis=0, tiled=True)
    arrived, gate_up, down = lax.optimization_barrier((arrived, gate_up, down))
    own_residual = lax.dynamic_slice_in_dim(residual, ep_rank * quarter, quarter, 1)
    hidden_state = (
        own_residual.astype(jnp.float32) + arrived.astype(jnp.float32).sum(axis=0)
    ).astype(jnp.bfloat16)

    experts = jnp.arange(SIDE, dtype=jnp.int32)
    logit_gap = route_logits[:, 1] - route_logits[:, 0]
    first_share = 1.0 / (1.0 + jnp.exp(logit_gap))
    second_share = 1.0 / (1.0 + jnp.exp(-logit_gap))
    names_first = expert_ids[:, 0][:, None] == experts[None, :]
    names_second = expert_ids[:, 1][:, None] == experts[None, :]
    member = (names_first | names_second).astype(jnp.int32)
    slot_index = jnp.cumsum(member, axis=0) - member
    share = jnp.where(names_first, first_share[:, None], 0.0) + jnp.where(
        names_second, second_share[:, None], 0.0
    )
    slot_ids = jnp.arange(CAP, dtype=jnp.int32)
    placed_at = (slot_index[:, :, None] == slot_ids[None, None, :]) & (member[:, :, None] == 1)
    selector = placed_at.astype(jnp.bfloat16).reshape(tokens, SIDE * CAP)
    mix_weight = jnp.where(placed_at, share[:, :, None], 0.0).reshape(tokens, SIDE * CAP)

    rows = lax.dot_general(
        selector, hidden_state, (((0,), (0,)), ((), ())), preferred_element_type=jnp.float32
    ).astype(jnp.bfloat16)
    rows = lax.all_to_all(
        rows.reshape(SIDE, CAP, quarter), "ep", split_axis=0, concat_axis=0, tiled=True
    )
    wide = rows.astype(jnp.float32)
    mean_square = jnp.sum(wide * wide, axis=(0, 2), keepdims=True) / width
    gain = norm_gain.reshape(SIDE, 1, quarter)
    packed = (wide * lax.rsqrt(mean_square + EPS) * gain).astype(jnp.bfloat16)
    first = jnp.concatenate([packed[0], packed[1]], axis=1)
    second = jnp.concatenate([packed[2], packed[3]], axis=1)

    first_line = gather_line(first, "y")
    second_line = gather_line(second, "z")
    first_all = gather_ring(
        jnp.concatenate(first_line[:2], axis=0), jnp.concatenate(first_line[2:], axis=0), "z"
    )
    second_all = gather_ring(
        jnp.concatenate(second_line[:2], axis=0), jnp.concatenate(second_line[2:], axis=0), "y"
    )

    units = down.shape[0]

    def lift(groups, weight):
        early = jnp.concatenate([groups[d][k] for d in (0, 1, 3) for k in (0, 1)], axis=0)
        late = jnp.concatenate(groups[2], axis=0)
        early = jnp.dot(early, weight, preferred_element_type=jnp.float32)
        late = jnp.dot(late, weight, preferred_element_type=jnp.float32)
        rows = late.shape[0]
        parts = [early[:rows], early[rows : 2 * rows], late, early[2 * rows :]]
        return jnp.stack([p.reshape(SIDE, CAP, 2 * units) for p in parts])

    lifted = lift(first_all, gate_up[:half]) + lift(second_all, gate_up[half:]).transpose(1, 0, 2, 3)
    hidden = (jax.nn.silu(lifted[..., :units]) * lifted[..., units:]).astype(jnp.bfloat16)

    def lower(hidden, weight):
        rows = SIDE * CAP
        late = jnp.concatenate([hidden[1], hidden[3], hidden[0]]).reshape(3 * rows, units)
        early = jnp.dot(
            hidden[2].reshape(rows, units), weight, preferred_element_type=jnp.float32
        ).astype(jnp.bfloat16)
        late = jnp.dot(late, weight, preferred_element_type=jnp.float32).astype(jnp.bfloat16)
        cut = rows // 2
        at = {1: 0, 3: rows, 0: 2 * rows}
        pieces = [None] * SIDE
        pieces[2] = (early[:cut], early[cut:])
        for d, start in at.items():
            pieces[d] = (late[start : start + cut], late[start + cut : start + rows])
        return pieces

    sum_first = scatter_line(*scatter_ring(lower(hidden, down[:, :half]), "z"), "y")
    sum_second = scatter_line(
        *scatter_ring(lower(hidden.transpose(1, 0, 2, 3), down[:, half:]), "y"), "z"
    )
    back = jnp.stack(
        [sum_first[:, :quarter], sum_first[:, quarter:], sum_second[:, :quarter], sum_second[:, quarter:]]
    )
    back = lax.all_to_all(back, "ep", split_axis=0, concat_axis=0, tiled=True)
    back = back.reshape(SIDE * CAP, quarter)
    high = mix_weight.astype(jnp.bfloat16)
    low = (mix_weight - high.astype(jnp.float32)).astype(jnp.bfloat16)
    mixed = jnp.dot(high, back, preferred_element_type=jnp.float32) + jnp.dot(
        low, back, preferred_element_type=jnp.float32
    )
    return (hidden_state, mixed.astype(jnp.bfloat16))


def solution(mesh):
    return jax.shard_map(
        local,
        mesh=mesh,
        in_specs=(
            P("cp", None),
            P("cp", "ep"),
            P("cp", "ep"),
            P("cp", "ep"),
            P("ep", None),
            P(),
            P(),
            P(),
            P("cp", None),
            P("cp", None),
            P("ep", None, "cp"),
            P("ep", None, "cp"),
            P("ep", "cp", None),
        ),
        out_specs=(P("cp", "ep"), P("cp", "ep")),
        check_vma=False,
    )
```

```python
import math

import jax
import jax.numpy as jnp
from jax import lax
from jax.experimental import pallas as pl
from jax.experimental.pallas import tpu as pltpu
from jax.sharding import PartitionSpec as P


HD = 128
CAP = 40
EPS = 1e-05
NEG = -1e30
SIDE = 4
WINDOW = 9


def device_at(y, z, core):
    return ((y % SIDE) * SIDE + z % SIDE) * 2 + core % 2


def shifted(array, dy, dz, dcore=0):
    pairs = [
        (device_at(y, z, c), device_at(y + dy, z + dz, c + dcore))
        for y in range(SIDE)
        for z in range(SIDE)
        for c in range(2)
    ]
    return lax.ppermute(array, "cp", pairs)


def along(array, dim, step):
    return shifted(array, step, 0) if dim == "y" else shifted(array, 0, step)


def gather_line(array, dim):
    return [array] + [along(array, dim, step) for step in (1, 2, 3)]


def attention_kernel(
    rank_ref, order_ref, q_ref, own_ref, other_ref, docs_ref, weight_hbm, out_ref,
    kv_ref, bias_ref, attended_ref, weight_ref, sems,
):
    tokens = q_ref.shape[0]
    heads = q_ref.shape[1] // HD
    quarters, _, quarter = out_ref.shape

    def fetch(j):
        return pltpu.make_async_copy(
            weight_hbm.at[:, pl.ds(j * quarter, quarter)], weight_ref.at[j], sems.at[j]
        )

    for j in range(quarters):
        fetch(j).start()

    rank = rank_ref[0]
    core = rank % 2
    z = (rank // 2) % SIDE
    y = rank // (2 * SIDE)
    placed = order_ref[rank]
    first_block = placed - (WINDOW - 1)

    def place_from(source, slot_core):
        def place(in_half, carry):
            slot_y = (y + SIDE - in_half % SIDE) % SIDE
            slot_z = (z + SIDE - in_half // SIDE) % SIDE
            at = order_ref[(slot_y * SIDE + slot_z) * 2 + slot_core] - first_block

            @pl.when((at >= 0) & (at < WINDOW))
            def _():
                kv_ref[pl.ds(pl.multiple_of(at * tokens, tokens), tokens), :] = source[
                    pl.ds(pl.multiple_of(in_half * tokens, tokens), tokens), :
                ]

            return carry

        lax.fori_loop(0, SIDE * SIDE, place, 0)

    place_from(own_ref, core)
    place_from(other_ref, 1 - core)

    row_at = lax.broadcasted_iota(jnp.int32, (tokens, tokens), 0)
    key_at = lax.broadcasted_iota(jnp.int32, (tokens, tokens), 1)
    own_docs = docs_ref[pl.ds(placed, 1), :]
    row_docs = jnp.sum(jnp.where(row_at == key_at, own_docs, 0), axis=1, keepdims=True)

    def mask(w, carry):
        block = first_block + w
        at = pl.ds(pl.multiple_of(w * tokens, tokens), tokens)

        @pl.when(block < 0)
        def _():
            kv_ref[at, :] = jnp.zeros((tokens, 2 * HD), jnp.bfloat16)

        allowed = docs_ref[pl.ds(jnp.maximum(block, 0), 1), :] == row_docs
        reach = jnp.where(block < 0, -2 * WINDOW * tokens, (WINDOW - 1 - w) * tokens)
        allowed = allowed & (key_at <= row_at + reach)
        bias_ref[:, at] = jnp.where(allowed, 0.0, NEG)
        return carry

    lax.fori_loop(0, WINDOW, mask, 0)

    def head(h, carry):
        at = pl.ds(pl.multiple_of(h * HD, HD), HD)
        scores = lax.dot_general(
            q_ref[:, at], kv_ref[:, :HD], (((1,), (1,)), ((), ())), preferred_element_type=jnp.float32
        )
        scores = scores * (1.0 / math.sqrt(HD)) + bias_ref[...]
        weights = jnp.exp(scores - jnp.max(scores, axis=1, keepdims=True))
        total = jnp.sum(weights, axis=1, keepdims=True)
        mix = jnp.dot(
            weights.astype(jnp.bfloat16), kv_ref[:, HD:], preferred_element_type=jnp.float32
        )
        attended_ref[:, at] = (mix / total).astype(jnp.bfloat16)
        return carry

    lax.fori_loop(0, heads, head, 0)
    for j in range(quarters):
        fetch(j).wait()
        out_ref[j] = jnp.dot(
            attended_ref[...], weight_ref[j], preferred_element_type=jnp.float32
        ).astype(jnp.bfloat16)


def attend_and_project(rank, order, queries, own, other, docs, out_weight):
    tokens, inner = queries.shape
    quarter = out_weight.shape[1] // SIDE
    smem = pl.BlockSpec(memory_space=pltpu.SMEM)
    vmem = pl.BlockSpec(memory_space=pltpu.VMEM)
    return pl.pallas_call(
        attention_kernel,
        out_shape=jax.ShapeDtypeStruct((SIDE, tokens, quarter), jnp.bfloat16),
        in_specs=[smem, smem, vmem, vmem, vmem, vmem, pl.BlockSpec(memory_space=pltpu.HBM)],
        out_specs=vmem,
        scratch_shapes=[
            pltpu.VMEM((WINDOW * tokens, 2 * HD), jnp.bfloat16),
            pltpu.VMEM((tokens, WINDOW * tokens), jnp.float32),
            pltpu.VMEM((tokens, inner), jnp.bfloat16),
            pltpu.VMEM((SIDE, inner, quarter), jnp.bfloat16),
            pltpu.SemaphoreType.DMA((SIDE,)),
        ],
        compiler_params=pltpu.CompilerParams(vmem_limit_bytes=48 * 1024 * 1024),
        name="attention",
    )(rank, order, queries, own, other, docs, out_weight)


TILE = 256


def tiles(width, body):
    def step(n, carry):
        body(pl.ds(pl.multiple_of(n * TILE, TILE), TILE), n)
        return carry

    lax.fori_loop(0, width // TILE, step, 0)


def lift_groups(groups, weight_ref, sums_ref, lanes):
    rows = 2 * groups[0][1].shape[0]
    inner = groups[0][1].shape[1]

    def body(cols, n):
        for lane, (d, near_ref, far_ref) in zip(lanes, groups):
            x = jnp.concatenate([near_ref[...], far_ref[...]], axis=0)
            sums_ref[lane, d * rows : (d + 1) * rows, cols] = jnp.dot(
                x,
                weight_ref[lane * inner : (lane + 1) * inner, cols],
                preferred_element_type=jnp.float32,
            )

    tiles(weight_ref.shape[1], body)


EARLY = (0, 1, 3)
LAST = 2


def early_kernel(*refs):
    *pieces, weight_ref, sums_ref = refs
    groups, lanes = [], []
    for lane in range(2):
        for k, d in enumerate(EARLY):
            at = 2 * (lane * len(EARLY) + k)
            groups.append((d, pieces[at], pieces[at + 1]))
            lanes.append(lane)
    lift_groups(groups, weight_ref, sums_ref, lanes)


def lower_groups(hidden_refs, down_ref, outs):
    rows = hidden_refs[0].shape[0] // SIDE
    half = outs[0][2].shape[1]

    def body(cols, n):
        for lane, d, near_ref, far_ref in outs:
            x = hidden_refs[lane][d * rows : (d + 1) * rows, :].astype(jnp.bfloat16)
            w = down_ref[:, pl.ds(pl.multiple_of(lane * half + n * TILE, TILE), TILE)]
            y = jnp.dot(x, w, preferred_element_type=jnp.float32).astype(jnp.bfloat16)
            near_ref[:, cols] = y[: rows // 2]
            far_ref[:, cols] = y[rows // 2 :]

    tiles(half, body)


def last_kernel(
    a_near, a_far, b_near, b_far, weight_ref, early_ref, down_ref,
    hidden_a, hidden_b, a_out_near, a_out_far, b_out_near, b_out_far, late_ref,
):
    rows = 2 * a_near.shape[0]
    units = down_ref.shape[0]
    slots = rows // SIDE
    lift_groups(
        [(0, a_near, a_far), (0, b_near, b_far)], weight_ref, late_ref, (0, 1)
    )

    def combine(a_ref, a_base, b_ref, b_base, a_group, b_group):
        a_at = pl.ds(pl.multiple_of(a_base + b_group * slots, 8), slots)
        b_at = pl.ds(pl.multiple_of(b_base + a_group * slots, 8), slots)
        gate = a_ref[0, a_at, :units] + b_ref[1, b_at, :units]
        up = a_ref[0, a_at, units:] + b_ref[1, b_at, units:]
        value = gate / (1.0 + jnp.exp(-gate)) * up
        hidden_a[pl.ds(pl.multiple_of(a_group * rows + b_group * slots, 8), slots), :] = value
        hidden_b[pl.ds(pl.multiple_of(b_group * rows + a_group * slots, 8), slots), :] = value

    combine(late_ref, 0, late_ref, 0, LAST, LAST)

    def each(k, carry):
        d = jnp.where(k == LAST, SIDE - 1, k)
        combine(late_ref, 0, early_ref, d * rows, LAST, d)
        combine(early_ref, d * rows, late_ref, 0, d, LAST)

        def other(m, inner):
            e = jnp.where(m == LAST, SIDE - 1, m)
            combine(early_ref, d * rows, early_ref, e * rows, d, e)
            return inner

        return lax.fori_loop(0, SIDE - 1, other, carry)

    lax.fori_loop(0, SIDE - 1, each, 0)
    lower_groups(
        (hidden_a, hidden_b),
        down_ref,
        [(0, LAST, a_out_near, a_out_far), (1, LAST, b_out_near, b_out_far)],
    )


def rest_kernel(hidden_a, hidden_b, down_ref, *outs):
    groups = []
    for lane in range(2):
        for k, d in enumerate(EARLY):
            at = 2 * (lane * len(EARLY) + k)
            groups.append((lane, d, outs[at], outs[at + 1]))
    lower_groups((hidden_a, hidden_b), down_ref, groups)


def in_vmem(kernel, out_shapes, operands, scratch=()):
    vmem = pl.BlockSpec(memory_space=pltpu.VMEM)
    return pl.pallas_call(
        kernel,
        out_shape=out_shapes,
        in_specs=[vmem] * len(operands),
        out_specs=[vmem] * len(out_shapes),
        scratch_shapes=list(scratch),
        compiler_params=pltpu.CompilerParams(vmem_limit_bytes=12 * 1024 * 1024),
    )(*operands)


def expert_parts(a_groups, b_groups, gate_up, down):
    piece = a_groups[0][0]
    rows = 2 * piece.shape[0]
    units, _ = down.shape
    early = [p for groups in (a_groups, b_groups) for d in EARLY for p in groups[d]]
    sums = jax.ShapeDtypeStruct((2, SIDE * rows, gate_up.shape[1]), jnp.float32)
    (early_sums,) = in_vmem(early_kernel, [sums], [*early, gate_up])
    hidden = jax.ShapeDtypeStruct((SIDE * rows, units), jnp.float32)
    part = jax.ShapeDtypeStruct(piece.shape, jnp.bfloat16)
    hidden_a, hidden_b, *first = in_vmem(
        last_kernel,
        [hidden, hidden] + [part] * 4,
        [*a_groups[LAST], *b_groups[LAST], gate_up, early_sums, down],
        [pltpu.VMEM((2, rows, gate_up.shape[1]), jnp.float32)],
    )
    rest = in_vmem(rest_kernel, [part] * (4 * len(EARLY)), [hidden_a, hidden_b, down])
    pieces = [[None] * SIDE, [None] * SIDE]
    for lane in range(2):
        pieces[lane][LAST] = (first[2 * lane], first[2 * lane + 1])
        for k, d in enumerate(EARLY):
            at = 2 * (lane * len(EARLY) + k)
            pieces[lane][d] = (rest[at], rest[at + 1])
    return pieces


def gather_ring(near, far, dim):
    up_near = along(near, dim, 1)
    down_far = along(far, dim, -1)
    up_far = along(far, dim, 1)
    down_near = along(near, dim, -1)
    two_near = along(up_near, dim, 1)
    two_far = along(down_far, dim, -1)
    return [(near, far), (up_near, up_far), (two_near, two_far), (down_near, down_far)]


def plus(*arrays):
    total = arrays[0].astype(jnp.float32)
    for a in arrays[1:]:
        total = total + a.astype(jnp.float32)
    return total.astype(jnp.bfloat16)


def scatter_ring(pieces, dim):
    near2 = along(pieces[2][0], dim, -1)
    far2 = along(pieces[2][1], dim, 1)
    far1 = along(pieces[1][1], dim, -1)
    near3 = along(pieces[3][0], dim, 1)
    near1 = along(plus(pieces[1][0], near2), dim, -1)
    far3 = along(plus(pieces[3][1], far2), dim, 1)
    near = plus(pieces[0][0], near3, near1)
    far = plus(pieces[0][1], far1, far3)
    return near, far


def scatter_line(near, far, dim):
    rows = near.shape[0] // 2
    pieces = [near[:rows], near[rows:], far[:rows], far[rows:]]
    moved = [along(pieces[step], dim, -step) for step in (1, 2, 3)]
    return plus(pieces[0], *moved)


def local(
    residual,
    queries,
    key_proj,
    value_proj,
    out_weight,
    norm_gain,
    doc_ids,
    block_order,
    expert_ids,
    route_logits,
    gate_weight,
    up_weight,
    down_weight,
):
    tokens, width = residual.shape
    quarter = width // SIDE
    cp_rank = lax.axis_index("cp")
    ep_rank = lax.axis_index("ep")

    gate_other = shifted(gate_weight[0], 0, 0, 1)
    up_other = shifted(up_weight[0], 0, 0, 1)
    down_other = shifted(down_weight[0], 0, 0, 1)

    kv = jnp.concatenate([key_proj, value_proj], axis=1)
    kv_line = jnp.concatenate(gather_line(kv, "y"), axis=0)
    kv_own = jnp.concatenate(gather_line(kv_line, "z"), axis=0)
    kv_other = shifted(kv_own, 0, 0, 1)

    projected = attend_and_project(
        cp_rank.reshape(1).astype(jnp.int32),
        block_order,
        queries,
        kv_own,
        kv_other,
        doc_ids.reshape(-1, tokens),
        out_weight,
    )
    gate_up = jnp.concatenate([gate_weight[0], gate_other, up_weight[0], up_other], axis=1)
    down = jnp.concatenate([down_weight[0], down_other], axis=0)
    arrived = lax.all_to_all(projected, "ep", split_axis=0, concat_axis=0, tiled=True)
    arrived, gate_up, down = lax.optimization_barrier((arrived, gate_up, down))
    own_residual = lax.dynamic_slice_in_dim(residual, ep_rank * quarter, quarter, 1)
    hidden_state = (
        own_residual.astype(jnp.float32) + arrived.astype(jnp.float32).sum(axis=0)
    ).astype(jnp.bfloat16)

    experts = jnp.arange(SIDE, dtype=jnp.int32)
    logit_gap = route_logits[:, 1] - route_logits[:, 0]
    first_share = 1.0 / (1.0 + jnp.exp(logit_gap))
    second_share = 1.0 / (1.0 + jnp.exp(-logit_gap))
    names_first = expert_ids[:, 0][:, None] == experts[None, :]
    names_second = expert_ids[:, 1][:, None] == experts[None, :]
    member = (names_first | names_second).astype(jnp.int32)
    slot_index = jnp.cumsum(member, axis=0) - member
    share = jnp.where(names_first, first_share[:, None], 0.0) + jnp.where(
        names_second, second_share[:, None], 0.0
    )
    slot_ids = jnp.arange(CAP, dtype=jnp.int32)
    placed_at = (slot_index[:, :, None] == slot_ids[None, None, :]) & (member[:, :, None] == 1)
    selector = placed_at.astype(jnp.bfloat16).reshape(tokens, SIDE * CAP)
    mix_weight = jnp.where(placed_at, share[:, :, None], 0.0).reshape(tokens, SIDE * CAP)

    rows = lax.dot_general(
        selector, hidden_state, (((0,), (0,)), ((), ())), preferred_element_type=jnp.float32
    ).astype(jnp.bfloat16)
    rows = lax.all_to_all(
        rows.reshape(SIDE, CAP, quarter), "ep", split_axis=0, concat_axis=0, tiled=True
    )
    wide = rows.astype(jnp.float32)
    mean_square = jnp.sum(wide * wide, axis=(0, 2), keepdims=True) / width
    gain = norm_gain.reshape(SIDE, 1, quarter)
    packed = (wide * lax.rsqrt(mean_square + EPS) * gain).astype(jnp.bfloat16)
    first = jnp.concatenate([packed[0], packed[1]], axis=1)
    second = jnp.concatenate([packed[2], packed[3]], axis=1)

    first_line = gather_line(first, "y")
    second_line = gather_line(second, "z")
    first_all = gather_ring(
        jnp.concatenate(first_line[:2], axis=0), jnp.concatenate(first_line[2:], axis=0), "z"
    )
    second_all = gather_ring(
        jnp.concatenate(second_line[:2], axis=0), jnp.concatenate(second_line[2:], axis=0), "y"
    )

    a_parts, b_parts = expert_parts(first_all, second_all, gate_up, down)
    sum_first = scatter_line(*scatter_ring(a_parts, "z"), "y")
    sum_second = scatter_line(*scatter_ring(b_parts, "y"), "z")
    back = jnp.stack(
        [sum_first[:, :quarter], sum_first[:, quarter:], sum_second[:, :quarter], sum_second[:, quarter:]]
    )
    back = lax.all_to_all(back, "ep", split_axis=0, concat_axis=0, tiled=True)
    back = back.reshape(SIDE * CAP, quarter)
    high = mix_weight.astype(jnp.bfloat16)
    low = (mix_weight - high.astype(jnp.float32)).astype(jnp.bfloat16)
    mixed = jnp.dot(high, back, preferred_element_type=jnp.float32) + jnp.dot(
        low, back, preferred_element_type=jnp.float32
    )
    return (hidden_state, mixed.astype(jnp.bfloat16))


def solution(mesh):
    return jax.shard_map(
        local,
        mesh=mesh,
        in_specs=(
            P("cp", None),
            P("cp", "ep"),
            P("cp", "ep"),
            P("cp", "ep"),
            P("ep", None),
            P(),
            P(),
            P(),
            P("cp", None),
            P("cp", None),
            P("ep", None, "cp"),
            P("ep", None, "cp"),
            P("ep", "cp", None),
        ),
        out_specs=(P("cp", "ep"), P("cp", "ep")),
        check_vma=False,
    )
```

```python
import math

import jax
import jax.numpy as jnp
from jax import lax
from jax.experimental import pallas as pl
from jax.experimental.pallas import tpu as pltpu
from jax.sharding import PartitionSpec as P


HD = 128
CAP = 40
EPS = 1e-05
NEG = -1e30
SIDE = 4
WINDOW = 9


def device_at(y, z, core):
    return ((y % SIDE) * SIDE + z % SIDE) * 2 + core % 2


def shifted(array, dy, dz, dcore=0):
    pairs = [
        (device_at(y, z, c), device_at(y + dy, z + dz, c + dcore))
        for y in range(SIDE)
        for z in range(SIDE)
        for c in range(2)
    ]
    return lax.ppermute(array, "cp", pairs)


def along(array, dim, step):
    if dim == "x":
        return lax.ppermute(array, "ep", [(i, (i + step) % SIDE) for i in range(SIDE)])
    return shifted(array, step, 0) if dim == "y" else shifted(array, 0, step)


def gather_line(array, dim):
    return [array] + [along(array, dim, step) for step in (1, 2, 3)]


def attention_kernel(
    rank_ref, order_ref, q_hbm, own_ref, other_ref, docs_hbm, weight_hbm, *rest
):
    *outs, q_ref, docs_ref, kv_ref, bias_ref, attended_ref, weight_ref, sems = rest
    tokens = q_ref.shape[0]
    heads = q_ref.shape[1] // HD
    quarter = weight_ref.shape[2]

    def fetch(d):
        at = ((rank_ref[1] + SIDE - d) % SIDE) * quarter
        return pltpu.make_async_copy(
            weight_hbm.at[:, pl.ds(pl.multiple_of(at, HD), quarter)], weight_ref.at[d], sems.at[d]
        )

    docs_copy = pltpu.make_async_copy(docs_hbm, docs_ref, sems.at[SIDE])
    q_copy = pltpu.make_async_copy(q_hbm, q_ref, sems.at[SIDE + 1])
    docs_copy.start()
    q_copy.start()
    for d in range(SIDE):
        fetch(d).start()

    rank = rank_ref[0]
    core = rank % 2
    z = (rank // 2) % SIDE
    y = rank // (2 * SIDE)
    placed = order_ref[rank]
    first_block = placed - (WINDOW - 1)

    def place_from(source, slot_core):
        def place(in_half, carry):
            slot_y = (y + SIDE - in_half % SIDE) % SIDE
            slot_z = (z + SIDE - in_half // SIDE) % SIDE
            at = order_ref[(slot_y * SIDE + slot_z) * 2 + slot_core] - first_block

            @pl.when((at >= 0) & (at < WINDOW))
            def _():
                kv_ref[pl.ds(pl.multiple_of(at * tokens, tokens), tokens), :] = source[
                    pl.ds(pl.multiple_of(in_half * tokens, tokens), tokens), :
                ]

            return carry

        lax.fori_loop(0, SIDE * SIDE, place, 0)

    place_from(own_ref, core)
    place_from(other_ref, 1 - core)

    docs_copy.wait()
    row_at = lax.broadcasted_iota(jnp.int32, (tokens, tokens), 0)
    key_at = lax.broadcasted_iota(jnp.int32, (tokens, tokens), 1)
    own_docs = docs_ref[pl.ds(placed, 1), :]
    row_docs = jnp.sum(jnp.where(row_at == key_at, own_docs, 0), axis=1, keepdims=True)

    def mask(w, carry):
        block = first_block + w
        at = pl.ds(pl.multiple_of(w * tokens, tokens), tokens)

        @pl.when(block < 0)
        def _():
            kv_ref[at, :] = jnp.zeros((tokens, 2 * HD), jnp.bfloat16)

        allowed = docs_ref[pl.ds(jnp.maximum(block, 0), 1), :] == row_docs
        reach = jnp.where(block < 0, -2 * WINDOW * tokens, (WINDOW - 1 - w) * tokens)
        allowed = allowed & (key_at <= row_at + reach)
        bias_ref[:, at] = jnp.where(allowed, 0.0, NEG)
        return carry

    lax.fori_loop(0, WINDOW, mask, 0)
    q_copy.wait()

    def head(h, carry):
        at = pl.ds(pl.multiple_of(h * HD, HD), HD)
        scores = lax.dot_general(
            q_ref[:, at], kv_ref[:, :HD], (((1,), (1,)), ((), ())), preferred_element_type=jnp.float32
        )
        scores = scores * (1.0 / math.sqrt(HD)) + bias_ref[...]
        weights = jnp.exp(scores - jnp.max(scores, axis=1, keepdims=True))
        total = jnp.sum(weights, axis=1, keepdims=True)
        mix = jnp.dot(
            weights.astype(jnp.bfloat16), kv_ref[:, HD:], preferred_element_type=jnp.float32
        )
        attended_ref[:, at] = (mix / total).astype(jnp.bfloat16)
        return carry

    lax.fori_loop(0, heads, head, 0)
    for d in range(SIDE):
        fetch(d).wait()
        part = jnp.dot(attended_ref[...], weight_ref[d], preferred_element_type=jnp.float32)
        part = part.astype(jnp.bfloat16)
        outs[2 * d][...] = part[: tokens // 2]
        outs[2 * d + 1][...] = part[tokens // 2 :]


def attend_and_project(ranks, order, queries, own, other, docs, out_weight):
    tokens, inner = queries.shape
    quarter = out_weight.shape[1] // SIDE
    smem = pl.BlockSpec(memory_space=pltpu.SMEM)
    vmem = pl.BlockSpec(memory_space=pltpu.VMEM)
    far = pl.BlockSpec(memory_space=pltpu.HBM)
    queries, docs, out_weight = in_hbm([queries, docs, out_weight])
    outs = pl.pallas_call(
        attention_kernel,
        out_shape=[jax.ShapeDtypeStruct((tokens // 2, quarter), jnp.bfloat16)] * (2 * SIDE),
        in_specs=[smem, smem, far, vmem, vmem, far, far],
        out_specs=[vmem] * (2 * SIDE),
        scratch_shapes=[
            pltpu.VMEM(queries.shape, queries.dtype),
            pltpu.VMEM(docs.shape, docs.dtype),
            pltpu.VMEM((WINDOW * tokens, 2 * HD), jnp.bfloat16),
            pltpu.VMEM((tokens, WINDOW * tokens), jnp.float32),
            pltpu.VMEM((tokens, inner), jnp.bfloat16),
            pltpu.VMEM((SIDE, inner, quarter), jnp.bfloat16),
            pltpu.SemaphoreType.DMA((SIDE + 2,)),
        ],
        compiler_params=pltpu.CompilerParams(vmem_limit_bytes=20 * 1024 * 1024),
        name="attention",
    )(ranks, order, queries, own, other, docs, out_weight)
    return [(outs[2 * d], outs[2 * d + 1]) for d in range(SIDE)]


TILE = 256
OWN_LIMIT = 12


def tiles(width, body):
    def step(n, carry):
        body(pl.ds(pl.multiple_of(n * TILE, TILE), TILE), n)
        return carry

    lax.fori_loop(0, width // TILE, step, 0)


def lift_groups(groups, weight_ref, sums_ref, arrive=None):
    rows = 2 * groups[0][2].shape[0]
    inner = groups[0][2].shape[1]

    def body(cols, n):
        if arrive is not None:
            arrive(n)
        for lane, k, near_ref, far_ref in groups:
            sums_ref[lane, k * rows : (k + 1) * rows, cols] = jnp.dot(
                jnp.concatenate([near_ref[...], far_ref[...]], axis=0),
                weight_ref[lane * inner : (lane + 1) * inner, cols],
                preferred_element_type=jnp.float32,
            )

    tiles(weight_ref.shape[1], body)


SIDES = (1, 3)
LAST = 2


def each_side(body):
    def step(k, carry):
        body(k, 2 * k + 1)
        return carry

    lax.fori_loop(0, len(SIDES), step, 0)


def combine(a_ref, a_at, b_ref, b_at, a_group, b_group, hidden_a, hidden_b):
    rows, units = hidden_a.shape[0] // SIDE, hidden_a.shape[1]
    slots = rows // SIDE

    def at(group, block):
        start = group * rows + block * slots
        return pl.ds(start if isinstance(start, int) else pl.multiple_of(start, 8), slots)

    a_rows, b_rows = at(a_at, b_group), at(b_at, a_group)
    gate = a_ref[0, a_rows, :units] + b_ref[1, b_rows, :units]
    up = a_ref[0, a_rows, units:] + b_ref[1, b_rows, units:]
    value = gate / (1.0 + jnp.exp(-gate)) * up
    hidden_a[at(a_group, b_group), :] = value
    hidden_b[at(b_group, a_group), :] = value


def own_kernel(*refs):
    pieces, lifts, downs = refs[:4], refs[4:8], refs[8:10]
    own_ref, weight_ref, down_ref, lift_sems, down_sems = refs[10:]
    units = downs[0].shape[0]

    def lift_copy(source, n):
        cols = pl.ds(pl.multiple_of(n * TILE, TILE), TILE)
        return pltpu.make_async_copy(source, weight_ref.at[:, cols], lift_sems.at[n])

    down_copies = [
        pltpu.make_async_copy(ref, down_ref.at[i * units : (i + 1) * units, :], down_sems.at[i])
        for i, ref in enumerate(downs)
    ]
    for n, ref in enumerate(lifts):
        lift_copy(ref, n).start()
    for copy in down_copies:
        copy.start()
    lift_groups(
        [(0, 0, pieces[0], pieces[1]), (1, 0, pieces[2], pieces[3])],
        weight_ref,
        own_ref,
        lambda n: lift_copy(lifts[0], n).wait(),
    )
    for copy in down_copies:
        copy.wait()


def early_kernel(*refs):
    pieces, own_ref, weight_ref, (sums_ref, hidden_a, hidden_b) = refs[:8], refs[8], refs[9], refs[10:]
    groups = []
    for lane in range(2):
        for k in range(len(SIDES)):
            at = 2 * (lane * len(SIDES) + k)
            groups.append((lane, k, pieces[at], pieces[at + 1]))
    lift_groups(groups, weight_ref, sums_ref)
    combine(own_ref, 0, own_ref, 0, 0, 0, hidden_a, hidden_b)

    def outer(k, d):
        combine(own_ref, 0, sums_ref, k, 0, d, hidden_a, hidden_b)
        combine(sums_ref, k, own_ref, 0, d, 0, hidden_a, hidden_b)
        each_side(
            lambda m, e: combine(sums_ref, k, sums_ref, m, d, e, hidden_a, hidden_b)
        )

    each_side(outer)


def lower_groups(hidden_refs, down_ref, outs):
    rows = hidden_refs[0].shape[0] // SIDE
    half = outs[0][2].shape[1]

    def body(cols, n):
        for lane, d, near_ref, far_ref in outs:
            x = hidden_refs[lane][d * rows : (d + 1) * rows, :].astype(jnp.bfloat16)
            w = down_ref[:, pl.ds(pl.multiple_of(lane * half + n * TILE, TILE), TILE)]
            y = jnp.dot(x, w, preferred_element_type=jnp.float32).astype(jnp.bfloat16)
            near_ref[:, cols] = y[: rows // 2]
            far_ref[:, cols] = y[rows // 2 :]

    tiles(half, body)


def last_kernel(
    a_near, a_far, b_near, b_far, weight_ref, own_ref, sums_ref, down_ref, early_a, early_b,
    hidden_a, hidden_b, a_out_near, a_out_far, b_out_near, b_out_far, late_ref,
):
    lift_groups([(0, 0, a_near, a_far), (1, 0, b_near, b_far)], weight_ref, late_ref)
    combine(late_ref, 0, late_ref, 0, LAST, LAST, hidden_a, hidden_b)
    combine(late_ref, 0, own_ref, 0, LAST, 0, hidden_a, hidden_b)
    combine(own_ref, 0, late_ref, 0, 0, LAST, hidden_a, hidden_b)

    def crossing(k, d):
        combine(late_ref, 0, sums_ref, k, LAST, d, hidden_a, hidden_b)
        combine(sums_ref, k, late_ref, 0, d, LAST, hidden_a, hidden_b)

    each_side(crossing)
    lower_groups(
        (hidden_a, hidden_b),
        down_ref,
        [(0, LAST, a_out_near, a_out_far), (1, LAST, b_out_near, b_out_far)],
    )


REST = (1, 3, 0)


def rest_kernel(hidden_a, hidden_b, down_ref, *outs):
    groups = []
    for lane in range(2):
        for k, d in enumerate(REST):
            at = 2 * (lane * len(REST) + k)
            groups.append((lane, d, outs[at], outs[at + 1]))
    lower_groups((hidden_a, hidden_b), down_ref, groups)


def in_hbm(arrays):
    return [pltpu.with_memory_space_constraint(a, pltpu.HBM) for a in arrays]


def in_vmem(kernel, out_shapes, operands, scratch=(), aliases=None, hbm=(), limit=12):
    vmem = pl.BlockSpec(memory_space=pltpu.VMEM)
    far = pl.BlockSpec(memory_space=pltpu.HBM)
    return pl.pallas_call(
        kernel,
        out_shape=out_shapes,
        in_specs=[far if i in hbm else vmem for i in range(len(operands))],
        out_specs=[vmem] * len(out_shapes),
        scratch_shapes=list(scratch),
        input_output_aliases=aliases or {},
        compiler_params=pltpu.CompilerParams(vmem_limit_bytes=limit * 1024 * 1024),
    )(*operands)


def expert_parts(a_groups, b_groups, lifts, downs):
    piece = a_groups[0][0]
    rows = 2 * piece.shape[0]
    units = 2 * downs[0].shape[0]
    both = 2 * units
    hidden = jax.ShapeDtypeStruct((SIDE * rows, units), jnp.float32)
    part = jax.ShapeDtypeStruct(piece.shape, jnp.bfloat16)
    own_sums, weight, down = in_vmem(
        own_kernel,
        [
            jax.ShapeDtypeStruct((2, rows, both), jnp.float32),
            jax.ShapeDtypeStruct((lifts[0].shape[0], both), piece.dtype),
            jax.ShapeDtypeStruct((units, downs[0].shape[1]), piece.dtype),
        ],
        [*a_groups[0], *b_groups[0], *in_hbm(lifts), *in_hbm(downs)],
        [pltpu.SemaphoreType.DMA((len(lifts),)), pltpu.SemaphoreType.DMA((len(downs),))],
        hbm=range(4, 10),
        limit=OWN_LIMIT,
    )
    sides = [p for groups in (a_groups, b_groups) for d in SIDES for p in groups[d]]
    sums, early_a, early_b = in_vmem(
        early_kernel,
        [jax.ShapeDtypeStruct((2, len(SIDES) * rows, both), jnp.float32), hidden, hidden],
        [*sides, own_sums, weight],
    )
    operands = [*a_groups[LAST], *b_groups[LAST], weight, own_sums, sums, down, early_a, early_b]
    hidden_a, hidden_b, *first = in_vmem(
        last_kernel,
        [hidden, hidden] + [part] * 4,
        operands,
        [pltpu.VMEM((2, rows, both), jnp.float32)],
        {len(operands) - 2: 0, len(operands) - 1: 1},
    )
    rest = in_vmem(rest_kernel, [part] * (4 * len(REST)), [hidden_a, hidden_b, down])
    pieces = [[None] * SIDE, [None] * SIDE]
    for lane in range(2):
        pieces[lane][LAST] = (first[2 * lane], first[2 * lane + 1])
        for k, d in enumerate(REST):
            at = 2 * (lane * len(REST) + k)
            pieces[lane][d] = (rest[at], rest[at + 1])
    return pieces


def gather_ring(near, far, dim):
    up_near = along(near, dim, 1)
    down_far = along(far, dim, -1)
    up_far = along(far, dim, 1)
    down_near = along(near, dim, -1)
    two_near = along(up_near, dim, 1)
    two_far = along(down_far, dim, -1)
    return [(near, far), (up_near, up_far), (two_near, two_far), (down_near, down_far)]


def plus(*arrays):
    total = arrays[0].astype(jnp.float32)
    for a in arrays[1:]:
        total = total + a.astype(jnp.float32)
    return total.astype(jnp.bfloat16)


def scatter_ring(pieces, dim):
    near2 = along(pieces[2][0], dim, -1)
    far2 = along(pieces[2][1], dim, 1)
    far1 = along(pieces[1][1], dim, -1)
    near3 = along(pieces[3][0], dim, 1)
    near1 = along(plus(pieces[1][0], near2), dim, -1)
    far3 = along(plus(pieces[3][1], far2), dim, 1)
    return (pieces[0][0], near3, near1), (pieces[0][1], far1, far3)


def summed_ring(pieces, dim):
    near, far = scatter_ring(pieces, dim)
    near = plus(*near)
    far = plus(*far)
    return near, far


def scatter_line(near, far, dim):
    rows = near.shape[0] // 2
    pieces = [near[:rows], near[rows:], far[:rows], far[rows:]]
    moved = [along(pieces[step], dim, -step) for step in (1, 2, 3)]
    return plus(pieces[0], *moved)


def local(
    residual,
    queries,
    key_proj,
    value_proj,
    out_weight,
    norm_gain,
    doc_ids,
    block_order,
    expert_ids,
    route_logits,
    gate_weight,
    up_weight,
    down_weight,
):
    tokens, width = residual.shape
    quarter = width // SIDE
    cp_rank = lax.axis_index("cp")
    ep_rank = lax.axis_index("ep")

    gate_other = shifted(gate_weight[0], 0, 0, 1)
    up_other = shifted(up_weight[0], 0, 0, 1)
    down_other = shifted(down_weight[0], 0, 0, 1)

    kv = jnp.concatenate([key_proj, value_proj], axis=1)
    kv_line = jnp.concatenate(gather_line(kv, "y"), axis=0)
    kv_own = jnp.concatenate(gather_line(kv_line, "z"), axis=0)
    kv_other = shifted(kv_own, 0, 0, 1)

    projected = attend_and_project(
        jnp.stack([cp_rank, ep_rank]).astype(jnp.int32),
        block_order,
        queries,
        kv_own,
        kv_other,
        doc_ids.reshape(-1, tokens),
        out_weight,
    )
    near, far = scatter_ring(projected, "x")
    own_residual = lax.dynamic_slice_in_dim(residual, ep_rank * quarter, quarter, 1)
    cut = tokens // 2
    hidden_near = plus(own_residual[:cut], *near)
    hidden_far = plus(own_residual[cut:], *far)
    hidden_state = jnp.concatenate([hidden_near, hidden_far], axis=0)

    experts = jnp.arange(SIDE, dtype=jnp.int32)
    logit_gap = route_logits[:, 1] - route_logits[:, 0]
    first_share = 1.0 / (1.0 + jnp.exp(logit_gap))
    second_share = 1.0 / (1.0 + jnp.exp(-logit_gap))
    names_first = expert_ids[:, 0][:, None] == experts[None, :]
    names_second = expert_ids[:, 1][:, None] == experts[None, :]
    member = (names_first | names_second).astype(jnp.int32)
    slot_index = jnp.cumsum(member, axis=0) - member
    share = jnp.where(names_first, first_share[:, None], 0.0) + jnp.where(
        names_second, second_share[:, None], 0.0
    )
    slot_ids = jnp.arange(CAP, dtype=jnp.int32)
    placed_at = (slot_index[:, :, None] == slot_ids[None, None, :]) & (member[:, :, None] == 1)
    selector = placed_at.astype(jnp.bfloat16).reshape(tokens, SIDE * CAP)
    mix_weight = jnp.where(placed_at, share[:, :, None], 0.0).reshape(tokens, SIDE * CAP)

    rows = lax.dot_general(
        selector, hidden_state, (((0,), (0,)), ((), ())), preferred_element_type=jnp.float32
    ).astype(jnp.bfloat16)
    rows = lax.all_to_all(
        rows.reshape(SIDE, CAP, quarter), "ep", split_axis=0, concat_axis=0, tiled=True
    )
    wide = rows.astype(jnp.float32)
    mean_square = jnp.sum(wide * wide, axis=(0, 2), keepdims=True) / width
    gain = norm_gain.reshape(SIDE, 1, quarter)
    packed = (wide * lax.rsqrt(mean_square + EPS) * gain).astype(jnp.bfloat16)
    first = jnp.concatenate([packed[0], packed[1]], axis=1)
    second = jnp.concatenate([packed[2], packed[3]], axis=1)

    first_line = gather_line(first, "y")
    second_line = gather_line(second, "z")
    first_all = gather_ring(
        jnp.concatenate(first_line[:2], axis=0), jnp.concatenate(first_line[2:], axis=0), "z"
    )
    second_all = gather_ring(
        jnp.concatenate(second_line[:2], axis=0), jnp.concatenate(second_line[2:], axis=0), "y"
    )

    a_parts, b_parts = expert_parts(
        first_all,
        second_all,
        (gate_weight[0], gate_other, up_weight[0], up_other),
        (down_weight[0], down_other),
    )
    sum_first = scatter_line(*summed_ring(a_parts, "z"), "y")
    sum_second = scatter_line(*summed_ring(b_parts, "y"), "z")
    back = jnp.stack(
        [sum_first[:, :quarter], sum_first[:, quarter:], sum_second[:, :quarter], sum_second[:, quarter:]]
    )
    back = lax.all_to_all(back, "ep", split_axis=0, concat_axis=0, tiled=True)
    back = back.reshape(SIDE * CAP, quarter)
    high = mix_weight.astype(jnp.bfloat16)
    low = (mix_weight - high.astype(jnp.float32)).astype(jnp.bfloat16)
    mixed = jnp.dot(high, back, preferred_element_type=jnp.float32) + jnp.dot(
        low, back, preferred_element_type=jnp.float32
    )
    return (hidden_state, mixed.astype(jnp.bfloat16))


def solution(mesh):
    return jax.shard_map(
        local,
        mesh=mesh,
        in_specs=(
            P("cp", None),
            P("cp", "ep"),
            P("cp", "ep"),
            P("cp", "ep"),
            P("ep", None),
            P(),
            P(),
            P(),
            P("cp", None),
            P("cp", None),
            P("ep", None, "cp"),
            P("ep", None, "cp"),
            P("ep", "cp", None),
        ),
        out_specs=(P("cp", "ep"), P("cp", "ep")),
        check_vma=False,
    )
```

```python
import math

import jax
import jax.numpy as jnp
from jax import lax
from jax.experimental import pallas as pl
from jax.experimental.pallas import tpu as pltpu
from jax.sharding import PartitionSpec as P


HD = 128
CAP = 40
EPS = 1e-05
NEG = -1e30
SIDE = 4
WINDOW = 9


def device_at(y, z, core):
    return ((y % SIDE) * SIDE + z % SIDE) * 2 + core % 2


def shifted(array, dy, dz, dcore=0):
    pairs = [
        (device_at(y, z, c), device_at(y + dy, z + dz, c + dcore))
        for y in range(SIDE)
        for z in range(SIDE)
        for c in range(2)
    ]
    return lax.ppermute(array, "cp", pairs)


def along(array, dim, step):
    if dim == "x":
        return lax.ppermute(array, "ep", [(i, (i + step) % SIDE) for i in range(SIDE)])
    return shifted(array, step, 0) if dim == "y" else shifted(array, 0, step)


def gather_line(array, dim):
    return [array] + [along(array, dim, step) for step in (1, 2, 3)]


def attention_kernel(
    place_ref, q_hbm, own_ref, other_ref, docs_hbm, weight_hbm, *rest
):
    *outs, q_ref, docs_ref, kv_ref, bias_ref, attended_ref, weight_ref, sems = rest
    tokens = q_ref.shape[0]
    heads = q_ref.shape[1] // HD
    quarter = weight_ref.shape[2]

    def fetch(d):
        at = ((place_ref[1] + SIDE - d) % SIDE) * quarter
        return pltpu.make_async_copy(
            weight_hbm.at[:, pl.ds(pl.multiple_of(at, HD), quarter)], weight_ref.at[d], sems.at[d]
        )

    docs_copy = pltpu.make_async_copy(docs_hbm, docs_ref, sems.at[SIDE])
    q_copy = pltpu.make_async_copy(q_hbm, q_ref, sems.at[SIDE + 1])
    docs_copy.start()
    q_copy.start()
    for d in range(SIDE):
        fetch(d).start()

    rank = place_ref[0]
    core = rank % 2
    z = (rank // 2) % SIDE
    y = rank // (2 * SIDE)
    placed = place_ref[2 + rank]
    first_block = placed - (WINDOW - 1)

    def place_from(source, slot_core):
        def place(in_half, carry):
            slot_y = (y + SIDE - in_half % SIDE) % SIDE
            slot_z = (z + SIDE - in_half // SIDE) % SIDE
            at = place_ref[2 + (slot_y * SIDE + slot_z) * 2 + slot_core] - first_block

            @pl.when((at >= 0) & (at < WINDOW))
            def _():
                kv_ref[pl.ds(pl.multiple_of(at * tokens, tokens), tokens), :] = source[
                    pl.ds(pl.multiple_of(in_half * tokens, tokens), tokens), :
                ]

            return carry

        lax.fori_loop(0, SIDE * SIDE, place, 0)

    place_from(own_ref, core)
    place_from(other_ref, 1 - core)

    docs_copy.wait()
    row_at = lax.broadcasted_iota(jnp.int32, (tokens, tokens), 0)
    key_at = lax.broadcasted_iota(jnp.int32, (tokens, tokens), 1)
    own_docs = docs_ref[pl.ds(placed, 1), :]
    row_docs = jnp.sum(jnp.where(row_at == key_at, own_docs, 0), axis=1, keepdims=True)

    def mask(w, carry):
        block = first_block + w
        at = pl.ds(pl.multiple_of(w * tokens, tokens), tokens)

        @pl.when(block < 0)
        def _():
            kv_ref[at, :] = jnp.zeros((tokens, 2 * HD), jnp.bfloat16)

        allowed = docs_ref[pl.ds(jnp.maximum(block, 0), 1), :] == row_docs
        reach = jnp.where(block < 0, -2 * WINDOW * tokens, (WINDOW - 1 - w) * tokens)
        allowed = allowed & (key_at <= row_at + reach)
        bias_ref[:, at] = jnp.where(allowed, 0.0, NEG)
        return carry

    lax.fori_loop(0, WINDOW, mask, 0)
    q_copy.wait()

    def head(h):
        at = slice(h * HD, (h + 1) * HD)
        scores = lax.dot_general(
            q_ref[:, at], kv_ref[:, :HD], (((1,), (1,)), ((), ())), preferred_element_type=jnp.float32
        )
        scores = scores * (1.0 / math.sqrt(HD)) + bias_ref[...]
        weights = jnp.exp(scores - jnp.max(scores, axis=1, keepdims=True))
        total = jnp.sum(weights, axis=1, keepdims=True)
        mix = jnp.dot(
            weights.astype(jnp.bfloat16), kv_ref[:, HD:], preferred_element_type=jnp.float32
        )
        attended_ref[:, at] = (mix / total).astype(jnp.bfloat16)

    for h in range(heads):
        head(h)
    for d in range(SIDE):
        fetch(d).wait()
        part = jnp.dot(attended_ref[...], weight_ref[d], preferred_element_type=jnp.float32)
        part = part.astype(jnp.bfloat16)
        outs[2 * d][...] = part[: tokens // 2]
        outs[2 * d + 1][...] = part[tokens // 2 :]


def attend_and_project(place, queries, own, other, docs, out_weight):
    tokens, inner = queries.shape
    quarter = out_weight.shape[1] // SIDE
    smem = pl.BlockSpec(memory_space=pltpu.SMEM)
    vmem = pl.BlockSpec(memory_space=pltpu.VMEM)
    far = pl.BlockSpec(memory_space=pltpu.HBM)
    queries, docs, out_weight = in_hbm([queries, docs, out_weight])
    outs = pl.pallas_call(
        attention_kernel,
        out_shape=[jax.ShapeDtypeStruct((tokens // 2, quarter), jnp.bfloat16)] * (2 * SIDE),
        in_specs=[smem, far, vmem, vmem, far, far],
        out_specs=[vmem] * (2 * SIDE),
        scratch_shapes=[
            pltpu.VMEM(queries.shape, queries.dtype),
            pltpu.VMEM(docs.shape, docs.dtype),
            pltpu.VMEM((WINDOW * tokens, 2 * HD), jnp.bfloat16),
            pltpu.VMEM((tokens, WINDOW * tokens), jnp.float32),
            pltpu.VMEM((tokens, inner), jnp.bfloat16),
            pltpu.VMEM((SIDE, inner, quarter), jnp.bfloat16),
            pltpu.SemaphoreType.DMA((SIDE + 2,)),
        ],
        compiler_params=pltpu.CompilerParams(vmem_limit_bytes=20 * 1024 * 1024),
        name="attention",
    )(place, queries, own, other, docs, out_weight)
    return [(outs[2 * d], outs[2 * d + 1]) for d in range(SIDE)]


TILE = 256


def tiles(width, body):
    def step(n, carry):
        body(pl.ds(pl.multiple_of(n * TILE, TILE), TILE), n)
        return carry

    lax.fori_loop(0, width // TILE, step, 0)


def lift_groups(groups, weight_ref, sums_ref, arrive=None):
    rows = 2 * groups[0][2].shape[0]
    inner = groups[0][2].shape[1]

    def body(cols, n):
        if arrive is not None:
            arrive(n)
        for lane, k, near_ref, far_ref in groups:
            sums_ref[lane, k * rows : (k + 1) * rows, cols] = jnp.dot(
                jnp.concatenate([near_ref[...], far_ref[...]], axis=0),
                weight_ref[lane * inner : (lane + 1) * inner, cols],
                preferred_element_type=jnp.float32,
            )

    tiles(weight_ref.shape[1], body)


SIDES = (1, 3)
LAST = 2


def each_side(body):
    def step(k, carry):
        body(k, 2 * k + 1)
        return carry

    lax.fori_loop(0, len(SIDES), step, 0)


def combine(a_ref, a_at, b_ref, b_at, a_group, b_group, hidden_a, hidden_b):
    rows, units = hidden_a.shape[0] // SIDE, hidden_a.shape[1]
    slots = rows // SIDE

    def at(group, block):
        start = group * rows + block * slots
        return pl.ds(start if isinstance(start, int) else pl.multiple_of(start, 8), slots)

    a_rows, b_rows = at(a_at, b_group), at(b_at, a_group)
    gate = a_ref[0, a_rows, :units] + b_ref[1, b_rows, :units]
    up = a_ref[0, a_rows, units:] + b_ref[1, b_rows, units:]
    value = gate / (1.0 + jnp.exp(-gate)) * up
    hidden_a[at(a_group, b_group), :] = value
    hidden_b[at(b_group, a_group), :] = value


def own_kernel(*refs):
    pieces, lifts, (own_ref, weight_ref, sems) = refs[:4], refs[4:8], refs[8:]

    def fetch(source, n):
        cols = pl.ds(pl.multiple_of(n * TILE, TILE), TILE)
        return pltpu.make_async_copy(source, weight_ref.at[:, cols], sems.at[n])

    for n, ref in enumerate(lifts):
        fetch(ref, n).start()
    lift_groups(
        [(0, 0, pieces[0], pieces[1]), (1, 0, pieces[2], pieces[3])],
        weight_ref,
        own_ref,
        lambda n: fetch(lifts[0], n).wait(),
    )


def early_kernel(*refs):
    pieces, own_ref, weight_ref, downs = refs[:8], refs[8], refs[9], refs[10:12]
    sums_ref, hidden_a, hidden_b, down_ref, sems = refs[12:]
    units = downs[0].shape[0]
    copies = [
        pltpu.make_async_copy(ref, down_ref.at[i * units : (i + 1) * units, :], sems.at[i])
        for i, ref in enumerate(downs)
    ]
    for copy in copies:
        copy.start()
    groups = []
    for lane in range(2):
        for k in range(len(SIDES)):
            at = 2 * (lane * len(SIDES) + k)
            groups.append((lane, k, pieces[at], pieces[at + 1]))
    lift_groups(groups, weight_ref, sums_ref)
    combine(own_ref, 0, own_ref, 0, 0, 0, hidden_a, hidden_b)

    def outer(k, d):
        combine(own_ref, 0, sums_ref, k, 0, d, hidden_a, hidden_b)
        combine(sums_ref, k, own_ref, 0, d, 0, hidden_a, hidden_b)
        each_side(
            lambda m, e: combine(sums_ref, k, sums_ref, m, d, e, hidden_a, hidden_b)
        )

    each_side(outer)
    for copy in copies:
        copy.wait()


def lower_groups(hidden_refs, down_ref, outs):
    rows = hidden_refs[0].shape[0] // SIDE
    half = outs[0][2].shape[1]

    def body(cols, n):
        for lane, d, near_ref, far_ref in outs:
            x = hidden_refs[lane][d * rows : (d + 1) * rows, :].astype(jnp.bfloat16)
            w = down_ref[:, pl.ds(pl.multiple_of(lane * half + n * TILE, TILE), TILE)]
            y = jnp.dot(x, w, preferred_element_type=jnp.float32).astype(jnp.bfloat16)
            near_ref[:, cols] = y[: rows // 2]
            far_ref[:, cols] = y[rows // 2 :]

    tiles(half, body)


def last_kernel(
    a_near, a_far, b_near, b_far, weight_ref, own_ref, sums_ref, down_ref, early_a, early_b,
    hidden_a, hidden_b, a_out_near, a_out_far, b_out_near, b_out_far, late_ref,
):
    lift_groups([(0, 0, a_near, a_far), (1, 0, b_near, b_far)], weight_ref, late_ref)
    combine(late_ref, 0, late_ref, 0, LAST, LAST, hidden_a, hidden_b)
    combine(late_ref, 0, own_ref, 0, LAST, 0, hidden_a, hidden_b)
    combine(own_ref, 0, late_ref, 0, 0, LAST, hidden_a, hidden_b)

    def crossing(k, d):
        combine(late_ref, 0, sums_ref, k, LAST, d, hidden_a, hidden_b)
        combine(sums_ref, k, late_ref, 0, d, LAST, hidden_a, hidden_b)

    each_side(crossing)
    lower_groups(
        (hidden_a, hidden_b),
        down_ref,
        [(0, LAST, a_out_near, a_out_far), (1, LAST, b_out_near, b_out_far)],
    )


REST = (1, 3, 0)


def rest_kernel(hidden_a, hidden_b, down_ref, *outs):
    groups = []
    for lane in range(2):
        for k, d in enumerate(REST):
            at = 2 * (lane * len(REST) + k)
            groups.append((lane, d, outs[at], outs[at + 1]))
    lower_groups((hidden_a, hidden_b), down_ref, groups)


def in_hbm(arrays):
    return [pltpu.with_memory_space_constraint(a, pltpu.HBM) for a in arrays]


def in_vmem(kernel, out_shapes, operands, scratch=(), aliases=None, hbm=()):
    vmem = pl.BlockSpec(memory_space=pltpu.VMEM)
    far = pl.BlockSpec(memory_space=pltpu.HBM)
    return pl.pallas_call(
        kernel,
        out_shape=out_shapes,
        in_specs=[far if i in hbm else vmem for i in range(len(operands))],
        out_specs=[vmem] * len(out_shapes),
        scratch_shapes=list(scratch),
        input_output_aliases=aliases or {},
        compiler_params=pltpu.CompilerParams(vmem_limit_bytes=12 * 1024 * 1024),
    )(*operands)


def expert_parts(a_groups, b_groups, lifts, downs):
    piece = a_groups[0][0]
    rows = 2 * piece.shape[0]
    units = 2 * downs[0].shape[0]
    both = 2 * units
    hidden = jax.ShapeDtypeStruct((SIDE * rows, units), jnp.float32)
    part = jax.ShapeDtypeStruct(piece.shape, jnp.bfloat16)
    own_sums, weight = in_vmem(
        own_kernel,
        [
            jax.ShapeDtypeStruct((2, rows, both), jnp.float32),
            jax.ShapeDtypeStruct((lifts[0].shape[0], both), piece.dtype),
        ],
        [*a_groups[0], *b_groups[0], *in_hbm(lifts)],
        [pltpu.SemaphoreType.DMA((len(lifts),))],
        hbm=range(4, 8),
    )
    sides = [p for groups in (a_groups, b_groups) for d in SIDES for p in groups[d]]
    sums, early_a, early_b, down = in_vmem(
        early_kernel,
        [
            jax.ShapeDtypeStruct((2, len(SIDES) * rows, both), jnp.float32),
            hidden,
            hidden,
            jax.ShapeDtypeStruct((units, downs[0].shape[1]), piece.dtype),
        ],
        [*sides, own_sums, weight, *in_hbm(downs)],
        [pltpu.SemaphoreType.DMA((len(downs),))],
        hbm=(10, 11),
    )
    operands = [*a_groups[LAST], *b_groups[LAST], weight, own_sums, sums, down, early_a, early_b]
    hidden_a, hidden_b, *first = in_vmem(
        last_kernel,
        [hidden, hidden] + [part] * 4,
        operands,
        [pltpu.VMEM((2, rows, both), jnp.float32)],
        {len(operands) - 2: 0, len(operands) - 1: 1},
    )
    rest = in_vmem(rest_kernel, [part] * (4 * len(REST)), [hidden_a, hidden_b, down])
    pieces = [[None] * SIDE, [None] * SIDE]
    for lane in range(2):
        pieces[lane][LAST] = (first[2 * lane], first[2 * lane + 1])
        for k, d in enumerate(REST):
            at = 2 * (lane * len(REST) + k)
            pieces[lane][d] = (rest[at], rest[at + 1])
    return pieces


def gather_ring(near, far, dim):
    up_near = along(near, dim, 1)
    down_far = along(far, dim, -1)
    up_far = along(far, dim, 1)
    down_near = along(near, dim, -1)
    two_near = along(up_near, dim, 1)
    two_far = along(down_far, dim, -1)
    return [(near, far), (up_near, up_far), (two_near, two_far), (down_near, down_far)]


def plus(*arrays):
    total = arrays[0].astype(jnp.float32)
    for a in arrays[1:]:
        total = total + a.astype(jnp.float32)
    return total.astype(jnp.bfloat16)


def scatter_ring(pieces, dim):
    near2 = along(pieces[2][0], dim, -1)
    far2 = along(pieces[2][1], dim, 1)
    far1 = along(pieces[1][1], dim, -1)
    near3 = along(pieces[3][0], dim, 1)
    near1 = along(plus(pieces[1][0], near2), dim, -1)
    far3 = along(plus(pieces[3][1], far2), dim, 1)
    return (pieces[0][0], near3, near1), (pieces[0][1], far1, far3)


def summed_ring(pieces, dim):
    near, far = scatter_ring(pieces, dim)
    near = plus(*near)
    far = plus(*far)
    return near, far


def scatter_line(near, far, dim):
    rows = near.shape[0] // 2
    pieces = [near[:rows], near[rows:], far[:rows], far[rows:]]
    moved = [along(pieces[step], dim, -step) for step in (1, 2, 3)]
    return plus(pieces[0], *moved)


def local(
    residual,
    queries,
    key_proj,
    value_proj,
    out_weight,
    norm_gain,
    doc_ids,
    block_order,
    expert_ids,
    route_logits,
    gate_weight,
    up_weight,
    down_weight,
):
    tokens, width = residual.shape
    quarter = width // SIDE
    cp_rank = lax.axis_index("cp")
    ep_rank = lax.axis_index("ep")

    gate_other = shifted(gate_weight[0], 0, 0, 1)
    up_other = shifted(up_weight[0], 0, 0, 1)
    down_other = shifted(down_weight[0], 0, 0, 1)

    kv = jnp.concatenate([key_proj, value_proj], axis=1)
    kv_line = jnp.concatenate(gather_line(kv, "y"), axis=0)
    kv_own = jnp.concatenate(gather_line(kv_line, "z"), axis=0)
    kv_other = shifted(kv_own, 0, 0, 1)

    projected = attend_and_project(
        jnp.concatenate([jnp.stack([cp_rank, ep_rank]).astype(jnp.int32), block_order]),
        queries,
        kv_own,
        kv_other,
        doc_ids.reshape(-1, tokens),
        out_weight,
    )
    near, far = scatter_ring(projected, "x")
    own_residual = lax.dynamic_slice_in_dim(residual, ep_rank * quarter, quarter, 1)
    cut = tokens // 2
    hidden_near = plus(own_residual[:cut], *near)
    hidden_far = plus(own_residual[cut:], *far)
    hidden_state = jnp.concatenate([hidden_near, hidden_far], axis=0)

    experts = jnp.arange(SIDE, dtype=jnp.int32)
    logit_gap = route_logits[:, 1] - route_logits[:, 0]
    first_share = 1.0 / (1.0 + jnp.exp(logit_gap))
    second_share = 1.0 / (1.0 + jnp.exp(-logit_gap))
    names_first = expert_ids[:, 0][:, None] == experts[None, :]
    names_second = expert_ids[:, 1][:, None] == experts[None, :]
    member = (names_first | names_second).astype(jnp.int32)
    slot_index = jnp.cumsum(member, axis=0) - member
    share = jnp.where(names_first, first_share[:, None], 0.0) + jnp.where(
        names_second, second_share[:, None], 0.0
    )
    slot_ids = jnp.arange(CAP, dtype=jnp.int32)
    placed_at = (slot_index[:, :, None] == slot_ids[None, None, :]) & (member[:, :, None] == 1)
    selector = placed_at.astype(jnp.bfloat16).reshape(tokens, SIDE * CAP)
    mix_weight = jnp.where(placed_at, share[:, :, None], 0.0).reshape(tokens, SIDE * CAP)

    rows = lax.dot_general(
        selector, hidden_state, (((0,), (0,)), ((), ())), preferred_element_type=jnp.float32
    ).astype(jnp.bfloat16)
    rows = lax.all_to_all(
        rows.reshape(SIDE, CAP, quarter), "ep", split_axis=0, concat_axis=0, tiled=True
    )
    wide = rows.astype(jnp.float32)
    mean_square = jnp.sum(wide * wide, axis=(0, 2), keepdims=True) / width
    gain = norm_gain.reshape(SIDE, 1, quarter)
    packed = (wide * lax.rsqrt(mean_square + EPS) * gain).astype(jnp.bfloat16)
    first = jnp.concatenate([packed[0], packed[1]], axis=1)
    second = jnp.concatenate([packed[2], packed[3]], axis=1)

    first_line = gather_line(first, "y")
    second_line = gather_line(second, "z")
    first_all = gather_ring(
        jnp.concatenate(first_line[:2], axis=0), jnp.concatenate(first_line[2:], axis=0), "z"
    )
    second_all = gather_ring(
        jnp.concatenate(second_line[:2], axis=0), jnp.concatenate(second_line[2:], axis=0), "y"
    )

    a_parts, b_parts = expert_parts(
        first_all,
        second_all,
        (gate_weight[0], gate_other, up_weight[0], up_other),
        (down_weight[0], down_other),
    )
    sum_first = scatter_line(*summed_ring(a_parts, "z"), "y")
    sum_second = scatter_line(*summed_ring(b_parts, "y"), "z")
    back = jnp.stack(
        [sum_first[:, :quarter], sum_first[:, quarter:], sum_second[:, :quarter], sum_second[:, quarter:]]
    )
    back = lax.all_to_all(back, "ep", split_axis=0, concat_axis=0, tiled=True)
    back = back.reshape(SIDE * CAP, quarter)
    high = mix_weight.astype(jnp.bfloat16)
    low = (mix_weight - high.astype(jnp.float32)).astype(jnp.bfloat16)
    mixed = jnp.dot(high, back, preferred_element_type=jnp.float32) + jnp.dot(
        low, back, preferred_element_type=jnp.float32
    )
    return (hidden_state, mixed.astype(jnp.bfloat16))


def solution(mesh):
    return jax.shard_map(
        local,
        mesh=mesh,
        in_specs=(
            P("cp", None),
            P("cp", "ep"),
            P("cp", "ep"),
            P("cp", "ep"),
            P("ep", None),
            P(),
            P(),
            P(),
            P("cp", None),
            P("cp", None),
            P("ep", None, "cp"),
            P("ep", None, "cp"),
            P("ep", "cp", None),
        ),
        out_specs=(P("cp", "ep"), P("cp", "ep")),
        check_vma=False,
    )
```

```python
import math

import jax
import jax.numpy as jnp
from jax import lax
from jax.experimental import pallas as pl
from jax.experimental.pallas import tpu as pltpu
from jax.sharding import PartitionSpec as P


HD = 128
CAP = 40
EPS = 1e-05
NEG = -1e30
SIDE = 4
WINDOW = 9


def device_at(y, z, core):
    return ((y % SIDE) * SIDE + z % SIDE) * 2 + core % 2


def shifted(array, dy, dz, dcore=0):
    pairs = [
        (device_at(y, z, c), device_at(y + dy, z + dz, c + dcore))
        for y in range(SIDE)
        for z in range(SIDE)
        for c in range(2)
    ]
    return lax.ppermute(array, "cp", pairs)


def along(array, dim, step):
    if dim == "x":
        return lax.ppermute(array, "ep", [(i, (i + step) % SIDE) for i in range(SIDE)])
    return shifted(array, step, 0) if dim == "y" else shifted(array, 0, step)


def gather_line(array, dim):
    return [array] + [along(array, dim, step) for step in (1, 2, 3)]


def attention_kernel(
    place_ref, q_hbm, own_ref, other_ref, docs_hbm, weight_hbm, *rest
):
    *outs, q_ref, docs_ref, kv_ref, bias_ref, attended_ref, weight_ref, sems = rest
    tokens = q_ref.shape[0]
    heads = q_ref.shape[1] // HD
    quarter = weight_ref.shape[2]

    def fetch(d):
        at = ((place_ref[1] + SIDE - d) % SIDE) * quarter
        return pltpu.make_async_copy(
            weight_hbm.at[:, pl.ds(pl.multiple_of(at, HD), quarter)], weight_ref.at[d], sems.at[d]
        )

    docs_copy = pltpu.make_async_copy(docs_hbm, docs_ref, sems.at[SIDE])
    q_copy = pltpu.make_async_copy(q_hbm, q_ref, sems.at[SIDE + 1])
    docs_copy.start()
    q_copy.start()
    for d in range(SIDE):
        fetch(d).start()

    rank = place_ref[0]
    core = rank % 2
    z = (rank // 2) % SIDE
    y = rank // (2 * SIDE)
    placed = place_ref[2 + rank]
    first_block = placed - (WINDOW - 1)

    def place_from(source, slot_core):
        def place(in_half, carry):
            slot_y = (y + SIDE - in_half % SIDE) % SIDE
            slot_z = (z + SIDE - in_half // SIDE) % SIDE
            at = place_ref[2 + (slot_y * SIDE + slot_z) * 2 + slot_core] - first_block

            @pl.when((at >= 0) & (at < WINDOW))
            def _():
                kv_ref[pl.ds(pl.multiple_of(at * tokens, tokens), tokens), :] = source[
                    pl.ds(pl.multiple_of(in_half * tokens, tokens), tokens), :
                ]

            return carry

        lax.fori_loop(0, SIDE * SIDE, place, 0)

    place_from(own_ref, core)
    place_from(other_ref, 1 - core)

    docs_copy.wait()
    row_at = lax.broadcasted_iota(jnp.int32, (tokens, tokens), 0)
    key_at = lax.broadcasted_iota(jnp.int32, (tokens, tokens), 1)
    own_docs = docs_ref[pl.ds(placed, 1), :]
    row_docs = jnp.sum(jnp.where(row_at == key_at, own_docs, 0), axis=1, keepdims=True)

    def mask(w, carry):
        block = first_block + w
        at = pl.ds(pl.multiple_of(w * tokens, tokens), tokens)

        @pl.when(block < 0)
        def _():
            kv_ref[at, :] = jnp.zeros((tokens, 2 * HD), jnp.bfloat16)

        allowed = docs_ref[pl.ds(jnp.maximum(block, 0), 1), :] == row_docs
        reach = jnp.where(block < 0, -2 * WINDOW * tokens, (WINDOW - 1 - w) * tokens)
        allowed = allowed & (key_at <= row_at + reach)
        bias_ref[:, at] = jnp.where(allowed, 0.0, NEG)
        return carry

    lax.fori_loop(0, WINDOW, mask, 0)
    q_copy.wait()

    def head(h):
        at = slice(h * HD, (h + 1) * HD)
        scores = lax.dot_general(
            q_ref[:, at], kv_ref[:, :HD], (((1,), (1,)), ((), ())), preferred_element_type=jnp.float32
        )
        scores = scores * (1.0 / math.sqrt(HD)) + bias_ref[...]
        weights = jnp.exp(scores - jnp.max(scores, axis=1, keepdims=True))
        total = jnp.sum(weights, axis=1, keepdims=True)
        mix = jnp.dot(
            weights.astype(jnp.bfloat16), kv_ref[:, HD:], preferred_element_type=jnp.float32
        )
        attended_ref[:, at] = (mix / total).astype(jnp.bfloat16)

    for h in range(heads):
        head(h)
    for d in range(SIDE):
        fetch(d).wait()
        part = jnp.dot(attended_ref[...], weight_ref[d], preferred_element_type=jnp.float32)
        part = part.astype(jnp.bfloat16)
        outs[2 * d][...] = part[: tokens // 2]
        outs[2 * d + 1][...] = part[tokens // 2 :]


def attend_and_project(place, queries, own, other, docs, out_weight):
    tokens, inner = queries.shape
    quarter = out_weight.shape[1] // SIDE
    smem = pl.BlockSpec(memory_space=pltpu.SMEM)
    vmem = pl.BlockSpec(memory_space=pltpu.VMEM)
    far = pl.BlockSpec(memory_space=pltpu.HBM)
    queries, docs, out_weight = in_hbm([queries, docs, out_weight])
    outs = pl.pallas_call(
        attention_kernel,
        out_shape=[jax.ShapeDtypeStruct((tokens // 2, quarter), jnp.bfloat16)] * (2 * SIDE),
        in_specs=[smem, far, vmem, vmem, far, far],
        out_specs=[vmem] * (2 * SIDE),
        scratch_shapes=[
            pltpu.VMEM(queries.shape, queries.dtype),
            pltpu.VMEM(docs.shape, docs.dtype),
            pltpu.VMEM((WINDOW * tokens, 2 * HD), jnp.bfloat16),
            pltpu.VMEM((tokens, WINDOW * tokens), jnp.float32),
            pltpu.VMEM((tokens, inner), jnp.bfloat16),
            pltpu.VMEM((SIDE, inner, quarter), jnp.bfloat16),
            pltpu.SemaphoreType.DMA((SIDE + 2,)),
        ],
        compiler_params=pltpu.CompilerParams(vmem_limit_bytes=20 * 1024 * 1024),
        name="attention",
    )(place, queries, own, other, docs, out_weight)
    return [(outs[2 * d], outs[2 * d + 1]) for d in range(SIDE)]


TILE = 256


def tiles(width, body):
    def step(n, carry):
        body(pl.ds(pl.multiple_of(n * TILE, TILE), TILE), n)
        return carry

    lax.fori_loop(0, width // TILE, step, 0)


def lift_groups(groups, weight_ref, sums_ref, arrive=None):
    rows = 2 * groups[0][2].shape[0]
    inner = groups[0][2].shape[1]

    def body(cols, n):
        if arrive is not None:
            arrive(n)
        for lane, k, near_ref, far_ref in groups:
            sums_ref[lane, k * rows : (k + 1) * rows, cols] = jnp.dot(
                jnp.concatenate([near_ref[...], far_ref[...]], axis=0),
                weight_ref[lane * inner : (lane + 1) * inner, cols],
                preferred_element_type=jnp.float32,
            )

    tiles(weight_ref.shape[1], body)


SIDES = (1, 3)
LAST = 2


def each_side(body):
    def step(k, carry):
        body(k, 2 * k + 1)
        return carry

    lax.fori_loop(0, len(SIDES), step, 0)


def combine(a_ref, a_at, b_ref, b_at, a_group, b_group, hidden_a, hidden_b):
    rows, units = hidden_a.shape[0] // SIDE, hidden_a.shape[1]
    slots = rows // SIDE

    def at(group, block):
        start = group * rows + block * slots
        return pl.ds(start if isinstance(start, int) else pl.multiple_of(start, 8), slots)

    a_rows, b_rows = at(a_at, b_group), at(b_at, a_group)
    gate = a_ref[0, a_rows, :units] + b_ref[1, b_rows, :units]
    up = a_ref[0, a_rows, units:] + b_ref[1, b_rows, units:]
    value = gate / (1.0 + jnp.exp(-gate)) * up
    hidden_a[at(a_group, b_group), :] = value
    hidden_b[at(b_group, a_group), :] = value


def own_kernel(*refs):
    pieces, lifts, (own_ref, weight_ref, sems) = refs[:4], refs[4:8], refs[8:]

    def fetch(source, n):
        cols = pl.ds(pl.multiple_of(n * TILE, TILE), TILE)
        return pltpu.make_async_copy(source, weight_ref.at[:, cols], sems.at[n])

    for n, ref in enumerate(lifts):
        fetch(ref, n).start()
    lift_groups(
        [(0, 0, pieces[0], pieces[1]), (1, 0, pieces[2], pieces[3])],
        weight_ref,
        own_ref,
        lambda n: fetch(lifts[0], n).wait(),
    )


def early_kernel(*refs):
    pieces, own_ref, weight_ref, downs = refs[:8], refs[8], refs[9], refs[10:12]
    sums_ref, hidden_a, hidden_b, down_ref, sems = refs[12:]
    units = downs[0].shape[0]
    copies = [
        pltpu.make_async_copy(ref, down_ref.at[i * units : (i + 1) * units, :], sems.at[i])
        for i, ref in enumerate(downs)
    ]
    for copy in copies:
        copy.start()
    groups = []
    for lane in range(2):
        for k in range(len(SIDES)):
            at = 2 * (lane * len(SIDES) + k)
            groups.append((lane, k, pieces[at], pieces[at + 1]))
    lift_groups(groups, weight_ref, sums_ref)
    combine(own_ref, 0, own_ref, 0, 0, 0, hidden_a, hidden_b)

    def outer(k, d):
        combine(own_ref, 0, sums_ref, k, 0, d, hidden_a, hidden_b)
        combine(sums_ref, k, own_ref, 0, d, 0, hidden_a, hidden_b)
        each_side(
            lambda m, e: combine(sums_ref, k, sums_ref, m, d, e, hidden_a, hidden_b)
        )

    each_side(outer)
    for copy in copies:
        copy.wait()


def lower_groups(hidden_refs, down_ref, outs):
    rows = hidden_refs[0].shape[0] // SIDE
    half = outs[0][2].shape[1]

    def body(cols, n):
        for lane, d, near_ref, far_ref in outs:
            x = hidden_refs[lane][d * rows : (d + 1) * rows, :].astype(jnp.bfloat16)
            w = down_ref[:, pl.ds(pl.multiple_of(lane * half + n * TILE, TILE), TILE)]
            y = jnp.dot(x, w, preferred_element_type=jnp.float32).astype(jnp.bfloat16)
            near_ref[:, cols] = y[: rows // 2]
            far_ref[:, cols] = y[rows // 2 :]

    tiles(half, body)


def late_kernel(near, far, weight_ref, late_ref):
    lift_groups([(0, 0, near, far)], weight_ref, late_ref)


def last_kernel(
    late_a, b_near, b_far, weight_ref, own_ref, sums_ref, down_ref, early_a, early_b,
    hidden_a, hidden_b, a_out_near, a_out_far, b_out_near, b_out_far, late_ref,
):
    lift_groups([(1, 0, b_near, b_far)], weight_ref, late_ref)
    combine(late_a, 0, late_ref, 0, LAST, LAST, hidden_a, hidden_b)
    combine(late_a, 0, own_ref, 0, LAST, 0, hidden_a, hidden_b)
    combine(own_ref, 0, late_ref, 0, 0, LAST, hidden_a, hidden_b)

    def crossing(k, d):
        combine(late_a, 0, sums_ref, k, LAST, d, hidden_a, hidden_b)
        combine(sums_ref, k, late_ref, 0, d, LAST, hidden_a, hidden_b)

    each_side(crossing)
    lower_groups(
        (hidden_a, hidden_b),
        down_ref,
        [(0, LAST, a_out_near, a_out_far), (1, LAST, b_out_near, b_out_far)],
    )


REST = (1, 3, 0)


def rest_kernel(hidden_a, hidden_b, down_ref, *outs):
    groups = []
    for lane in range(2):
        for k, d in enumerate(REST):
            at = 2 * (lane * len(REST) + k)
            groups.append((lane, d, outs[at], outs[at + 1]))
    lower_groups((hidden_a, hidden_b), down_ref, groups)


def in_hbm(arrays):
    return [pltpu.with_memory_space_constraint(a, pltpu.HBM) for a in arrays]


def in_vmem(kernel, out_shapes, operands, scratch=(), aliases=None, hbm=()):
    vmem = pl.BlockSpec(memory_space=pltpu.VMEM)
    far = pl.BlockSpec(memory_space=pltpu.HBM)
    return pl.pallas_call(
        kernel,
        out_shape=out_shapes,
        in_specs=[far if i in hbm else vmem for i in range(len(operands))],
        out_specs=[vmem] * len(out_shapes),
        scratch_shapes=list(scratch),
        input_output_aliases=aliases or {},
        compiler_params=pltpu.CompilerParams(vmem_limit_bytes=12 * 1024 * 1024),
    )(*operands)


def expert_parts(a_groups, b_groups, lifts, downs):
    piece = a_groups[0][0]
    rows = 2 * piece.shape[0]
    units = 2 * downs[0].shape[0]
    both = 2 * units
    hidden = jax.ShapeDtypeStruct((SIDE * rows, units), jnp.float32)
    part = jax.ShapeDtypeStruct(piece.shape, jnp.bfloat16)
    own_sums, weight = in_vmem(
        own_kernel,
        [
            jax.ShapeDtypeStruct((2, rows, both), jnp.float32),
            jax.ShapeDtypeStruct((lifts[0].shape[0], both), piece.dtype),
        ],
        [*a_groups[0], *b_groups[0], *in_hbm(lifts)],
        [pltpu.SemaphoreType.DMA((len(lifts),))],
        hbm=range(4, 8),
    )
    sides = [p for groups in (a_groups, b_groups) for d in SIDES for p in groups[d]]
    sums, early_a, early_b, down = in_vmem(
        early_kernel,
        [
            jax.ShapeDtypeStruct((2, len(SIDES) * rows, both), jnp.float32),
            hidden,
            hidden,
            jax.ShapeDtypeStruct((units, downs[0].shape[1]), piece.dtype),
        ],
        [*sides, own_sums, weight, *in_hbm(downs)],
        [pltpu.SemaphoreType.DMA((len(downs),))],
        hbm=(10, 11),
    )
    (late_a,) = in_vmem(
        late_kernel, [jax.ShapeDtypeStruct((1, rows, both), jnp.float32)], [*a_groups[LAST], weight]
    )
    operands = [late_a, *b_groups[LAST], weight, own_sums, sums, down, early_a, early_b]
    hidden_a, hidden_b, *first = in_vmem(
        last_kernel,
        [hidden, hidden] + [part] * 4,
        operands,
        [pltpu.VMEM((2, rows, both), jnp.float32)],
        {len(operands) - 2: 0, len(operands) - 1: 1},
    )
    rest = in_vmem(rest_kernel, [part] * (4 * len(REST)), [hidden_a, hidden_b, down])
    pieces = [[None] * SIDE, [None] * SIDE]
    for lane in range(2):
        pieces[lane][LAST] = (first[2 * lane], first[2 * lane + 1])
        for k, d in enumerate(REST):
            at = 2 * (lane * len(REST) + k)
            pieces[lane][d] = (rest[at], rest[at + 1])
    return pieces


def gather_ring(near, far, dim):
    up_near = along(near, dim, 1)
    down_far = along(far, dim, -1)
    up_far = along(far, dim, 1)
    down_near = along(near, dim, -1)
    two_near = along(up_near, dim, 1)
    two_far = along(down_far, dim, -1)
    return [(near, far), (up_near, up_far), (two_near, two_far), (down_near, down_far)]


def plus(*arrays):
    total = arrays[0].astype(jnp.float32)
    for a in arrays[1:]:
        total = total + a.astype(jnp.float32)
    return total.astype(jnp.bfloat16)


def scatter_ring(pieces, dim):
    near2 = along(pieces[2][0], dim, -1)
    far2 = along(pieces[2][1], dim, 1)
    far1 = along(pieces[1][1], dim, -1)
    near3 = along(pieces[3][0], dim, 1)
    near1 = along(plus(pieces[1][0], near2), dim, -1)
    far3 = along(plus(pieces[3][1], far2), dim, 1)
    return (pieces[0][0], near3, near1), (pieces[0][1], far1, far3)


def summed_ring(pieces, dim):
    near, far = scatter_ring(pieces, dim)
    near = plus(*near)
    far = plus(*far)
    return near, far


def scatter_line(near, far, dim):
    rows = near.shape[0] // 2
    pieces = [near[:rows], near[rows:], far[:rows], far[rows:]]
    moved = [along(pieces[step], dim, -step) for step in (1, 2, 3)]
    return plus(pieces[0], *moved)


def local(
    residual,
    queries,
    key_proj,
    value_proj,
    out_weight,
    norm_gain,
    doc_ids,
    block_order,
    expert_ids,
    route_logits,
    gate_weight,
    up_weight,
    down_weight,
):
    tokens, width = residual.shape
    quarter = width // SIDE
    cp_rank = lax.axis_index("cp")
    ep_rank = lax.axis_index("ep")

    gate_other = shifted(gate_weight[0], 0, 0, 1)
    up_other = shifted(up_weight[0], 0, 0, 1)
    down_other = shifted(down_weight[0], 0, 0, 1)

    kv = jnp.concatenate([key_proj, value_proj], axis=1)
    kv_line = jnp.concatenate(gather_line(kv, "y"), axis=0)
    kv_own = jnp.concatenate(gather_line(kv_line, "z"), axis=0)
    kv_other = shifted(kv_own, 0, 0, 1)

    projected = attend_and_project(
        jnp.concatenate([jnp.stack([cp_rank, ep_rank]).astype(jnp.int32), block_order]),
        queries,
        kv_own,
        kv_other,
        doc_ids.reshape(-1, tokens),
        out_weight,
    )
    near, far = scatter_ring(projected, "x")
    own_residual = lax.dynamic_slice_in_dim(residual, ep_rank * quarter, quarter, 1)
    cut = tokens // 2
    hidden_near = plus(own_residual[:cut], *near)
    hidden_far = plus(own_residual[cut:], *far)
    hidden_state = jnp.concatenate([hidden_near, hidden_far], axis=0)

    experts = jnp.arange(SIDE, dtype=jnp.int32)
    logit_gap = route_logits[:, 1] - route_logits[:, 0]
    first_share = 1.0 / (1.0 + jnp.exp(logit_gap))
    second_share = 1.0 / (1.0 + jnp.exp(-logit_gap))
    names_first = expert_ids[:, 0][:, None] == experts[None, :]
    names_second = expert_ids[:, 1][:, None] == experts[None, :]
    member = (names_first | names_second).astype(jnp.int32)
    slot_index = jnp.cumsum(member, axis=0) - member
    share = jnp.where(names_first, first_share[:, None], 0.0) + jnp.where(
        names_second, second_share[:, None], 0.0
    )
    slot_ids = jnp.arange(CAP, dtype=jnp.int32)
    placed_at = (slot_index[:, :, None] == slot_ids[None, None, :]) & (member[:, :, None] == 1)
    selector = placed_at.astype(jnp.bfloat16).reshape(tokens, SIDE * CAP)
    mix_weight = jnp.where(placed_at, share[:, :, None], 0.0).reshape(tokens, SIDE * CAP)

    rows = lax.dot_general(
        selector, hidden_state, (((0,), (0,)), ((), ())), preferred_element_type=jnp.float32
    ).astype(jnp.bfloat16)
    rows = lax.all_to_all(
        rows.reshape(SIDE, CAP, quarter), "ep", split_axis=0, concat_axis=0, tiled=True
    )
    wide = rows.astype(jnp.float32)
    mean_square = jnp.sum(wide * wide, axis=(0, 2), keepdims=True) / width
    gain = norm_gain.reshape(SIDE, 1, quarter)
    packed = (wide * lax.rsqrt(mean_square + EPS) * gain).astype(jnp.bfloat16)
    first = jnp.concatenate([packed[0], packed[1]], axis=1)
    second = jnp.concatenate([packed[2], packed[3]], axis=1)

    first_line = gather_line(first, "y")
    second_line = gather_line(second, "z")
    first_all = gather_ring(
        jnp.concatenate(first_line[:2], axis=0), jnp.concatenate(first_line[2:], axis=0), "z"
    )
    second_all = gather_ring(
        jnp.concatenate(second_line[:2], axis=0), jnp.concatenate(second_line[2:], axis=0), "y"
    )

    a_parts, b_parts = expert_parts(
        first_all,
        second_all,
        (gate_weight[0], gate_other, up_weight[0], up_other),
        (down_weight[0], down_other),
    )
    sum_first = scatter_line(*summed_ring(a_parts, "z"), "y")
    sum_second = scatter_line(*summed_ring(b_parts, "y"), "z")
    back = jnp.stack(
        [sum_first[:, :quarter], sum_first[:, quarter:], sum_second[:, :quarter], sum_second[:, quarter:]]
    )
    back = lax.all_to_all(back, "ep", split_axis=0, concat_axis=0, tiled=True)
    back = back.reshape(SIDE * CAP, quarter)
    high = mix_weight.astype(jnp.bfloat16)
    low = (mix_weight - high.astype(jnp.float32)).astype(jnp.bfloat16)
    mixed = jnp.dot(high, back, preferred_element_type=jnp.float32) + jnp.dot(
        low, back, preferred_element_type=jnp.float32
    )
    return (hidden_state, mixed.astype(jnp.bfloat16))


def solution(mesh):
    return jax.shard_map(
        local,
        mesh=mesh,
        in_specs=(
            P("cp", None),
            P("cp", "ep"),
            P("cp", "ep"),
            P("cp", "ep"),
            P("ep", None),
            P(),
            P(),
            P(),
            P("cp", None),
            P("cp", None),
            P("ep", None, "cp"),
            P("ep", None, "cp"),
            P("ep", "cp", None),
        ),
        out_specs=(P("cp", "ep"), P("cp", "ep")),
        check_vma=False,
    )
```
